768 devices in a mesh: section: 32 (over x_hi, y, core), tensor: 24 (over z, x_lo).
Axes of the slice: x: 4 (x_hi: 2, x_lo: 2; x = x_hi * 2 + x_lo), y: 8, z: 12, core: 2. Of those that a mesh axis runs over, the one named last changes fastest.
Arguments:
- section_inputs: bfloat16 [32, 3072, 1024], P('section', 'tensor'), may hold values from -6 to 6
- w_in: bfloat16 [32, 2304, 1024], P('section', 'tensor'), may hold values from -0.1875 to 0.1875
- in_bias: bfloat16 [32, 2304], P('section', 'tensor'), may hold values from -3 to 3
- w_out: bfloat16 [32, 2304, 1024], P('section', 'tensor'), may hold values from -0.125 to 0.125
- out_bias: float32 [32, 1024], P('section'), may hold values from -2 to 2
- norm_gain: float32 [32, 1024], P('section'), may hold values from 0.1 to 1.9
- norm_bias: float32 [32, 1024], P('section'), may hold values from -2 to 2
- patches: bfloat16 [8, 3072, 1024], P(None, 'tensor'), may hold values from -6 to 6
- plan: int32 [3], replicated, may hold values from 0 to 7, as said below
Outputs:
- received: bfloat16 [32, 4, 3072, 1024], P('section', None, 'tensor')
The draws below stay inside these ranges and needn't reach their ends.
Inputs may be any that keep to these rules, and one draw needn't show every extreme that they name: `plan`: the first min(8, 3) entries are all different.
All inputs are finite; a program needn't handle non-finite values.
Results may differ from the reference program's by a relative error of at most 0.0065.
Values may be sent and summed in bfloat16 or wider, within the bound.
A program may use at most 64 MiB of HBM per device.

```python
import jax
import jax.numpy as jnp
from jax import lax

D = 1024
FF = 2304
TICKS = 4
MICRO = 8
TOKG = 3072
N_SECTION = 32


def draw_plan(key, part):
    order = jax.random.permutation(key, MICRO).astype(jnp.int32)
    places = jnp.arange(TICKS - 1, dtype=jnp.int32) % MICRO
    return order[places].astype(jnp.int32)


def block_scale(key, shape, shards, least, largest):
    def one(position, parts):
        heights = jax.random.uniform(jax.random.fold_in(jax.random.fold_in(key, 6), position), (parts,), jnp.float32, least / len(shards), largest / len(shards))
        return jnp.repeat(jnp.exp(heights), shape[position] // parts).reshape((-1,) + (1,) * (len(shape) - position - 1))

    level = one(*shards[0])
    for cut in shards[1:]:
        level = level * one(*cut)
    return level


def noise(own_key, shape, scale, reach, shards=(), held_as=jnp.bfloat16):
    factor_of = block_scale(own_key, shape, shards, -0.22, 0.18) if shards else 1.0
    array = jax.random.normal(own_key, shape, jnp.float32) * scale * factor_of
    return jnp.minimum(jnp.maximum(array, -reach), reach).astype(held_as)


def setup_inputs(seed: int = 0) -> dict:
    key_of = jax.random.split(jax.random.key(seed), 10)
    section_inputs = noise(key_of[0], (N_SECTION, TOKG, D), 1.0, 6.0, ((0, 32), (1, 24)))
    w_in = noise(key_of[1], (N_SECTION, FF, D), D ** -0.5, 0.1875, ((0, 32), (1, 24)))
    in_bias = noise(key_of[2], (N_SECTION, FF), 0.5, 3.0, ((0, 32), (1, 24)))
    w_out = noise(key_of[3], (N_SECTION, FF, D), FF ** -0.5, 0.125, ((0, 32), (1, 24)))
    out_bias = noise(key_of[4], (N_SECTION, D), 0.3, 2.0, ((0, 32),), jnp.float32)
    norm_gain = jnp.clip(1.0 + 0.18 * jax.random.normal(key_of[5], (N_SECTION, D), jnp.float32), 0.1, 1.9)
    norm_bias = noise(key_of[6], (N_SECTION, D), 0.3, 2.0, ((0, 32),), jnp.float32)
    patches = noise(key_of[7], (MICRO, TOKG, D), 1.0, 6.0, ((1, 24),))
    plan = draw_plan(jax.random.fold_in(key_of[9], 71), 0)
    return {"section_inputs": section_inputs, "w_in": w_in, "in_bias": in_bias, "w_out": w_out, "out_bias": out_bias, "norm_gain": norm_gain, "norm_bias": norm_bias, "patches": patches, "plan": plan}


norm_floor = 0.1
gelu_slope = 1.702

def normalize(current, gain_row, shift_row):
    widened = current.astype(jnp.float32)
    average = lax.optimization_barrier(jnp.mean(widened, axis=-1, keepdims=True))
    centered = widened - average
    variance = lax.optimization_barrier(jnp.mean(centered * centered, axis=-1, keepdims=True))
    normed = (centered * lax.rsqrt(variance + norm_floor) * gain_row + shift_row).astype(jnp.bfloat16)
    return (normed, widened)

def activate(preact):
    return preact * jax.nn.sigmoid(gelu_slope * preact)

def apply_block(current, gain_row, shift_row, full_in, full_bias, full_out, bias_row):
    normed, widened = normalize(current, gain_row, shift_row)
    preact = lax.dot_general(normed, full_in, (((1,), (1,)), ((), ())), preferred_element_type=jnp.float32)
    preact = preact + full_bias.astype(jnp.float32)
    hidden = activate(preact).astype(jnp.bfloat16)
    return (widened + jnp.dot(hidden, full_out, preferred_element_type=jnp.float32) + bias_row).astype(jnp.bfloat16)

def reference(section_inputs, w_in, in_bias, w_out, out_bias, norm_gain, norm_bias, patches, plan):
    current = section_inputs
    records = []
    for tick_index in range(TICKS):
        produced = lax.map(lambda operands: apply_block(*operands), (current, norm_gain, norm_bias, w_in, in_bias, w_out, out_bias))
        arrived = jnp.roll(produced, 1, axis=0)
        records.append(arrived)
        if tick_index + 1 < TICKS:
            selected = lax.dynamic_index_in_dim(patches, plan[tick_index], 0, keepdims=False)
            current = arrived.at[0].set(selected)
    return jnp.stack(records, axis=1)
```

```python
import functools

import jax
import jax.numpy as jnp
from jax import lax
from jax.experimental import pallas as pl
from jax.experimental.pallas import tpu as pltpu
from jax.sharding import PartitionSpec as P

TICKS = 4
CHUNKS = 2
MESH = pl.DeviceIdType.MESH

norm_floor = 0.1
gelu_slope = 1.702

BIAS, W_IN, W_OUT = 0, 1, 2


def normalize(current, gain_row, shift_row):
    widened = current.astype(jnp.float32)
    average = jnp.mean(widened, axis=-1, keepdims=True)
    centered = widened - average
    variance = jnp.mean(centered * centered, axis=-1, keepdims=True)
    normed = (centered * lax.rsqrt(variance + norm_floor) * gain_row + shift_row).astype(
        jnp.bfloat16
    )
    return (normed, widened)


def activate(preact):
    return preact * jax.nn.sigmoid(gelu_slope * preact)


def rows_times(normed, rows):
    return lax.dot_general(
        normed, rows, (((1,), (1,)), ((), ())), preferred_element_type=jnp.float32
    )


def block_kernel(
    yn, zn,
    x_in, w_in, w_out, small_in, patches_in, plan, out,
    x0, win, wout, small, bias, bias_row, pat, sel, sel_far, cur, normed0, acc, hid, prod, arr,
    own_sem, own_send, ring_send, ring_recv, core_send, core_recv,
    pat_sem, sel_send, sel_recv, hop_send, hop_recv, back_send, back_recv,
):
    section = lax.axis_index("section")
    tensor = lax.axis_index("tensor")
    k = lax.rem(section, 2)
    y = lax.div(section, 2)
    r = lax.rem(tensor, 2)
    z = lax.div(tensor, 2)
    tokens, depth = x0.shape
    shard = w_in.shape[1]
    width = win.shape[0]
    half = zn // 2
    rows = tokens // CHUNKS

    def device(y, k, z, r):
        return (2 * y + k, 2 * z + r)

    up = device(y, k, lax.rem(z + 1, zn), r)
    down = device(y, k, lax.rem(z + zn - 1, zn), r)
    sibling = device(y, 1 - k, z, r)
    swapped = device(y, r, z, k)
    after = device(lax.rem(y + r, yn), k, z, 1 - r)
    before = device(lax.rem(y + yn - 1 + r, yn), k, z, 1 - r)
    last_to = device(lax.rem(y + r, yn), 1 - r, z, k)
    last_from = device(lax.rem(y + yn - 1 + k, yn), r, z, 1 - k)
    stays = r == k
    moves = r != k

    def slot_ref(piece, slot):
        if piece == BIAS:
            return bias.at[slot]
        whole = win if piece == W_IN else wout
        return whole.at[pl.ds(pl.multiple_of(slot * shard, shard), shard)]

    own = 2 * z + k
    sources = (small_in.at[:, pl.ds(0, 128)], w_in.at[0], w_out.at[0], small_in, x_in.at[0])

    def own_targets(slot):
        return (slot_ref(BIAS, slot), slot_ref(W_IN, slot), slot_ref(W_OUT, slot), small, x0)

    def own_local(i):
        return pltpu.make_async_copy(sources[i], own_targets(own)[i], own_sem.at[i])

    def own_remote(i, slot):
        return pltpu.make_async_remote_copy(
            src_ref=sources[i],
            dst_ref=own_targets(slot)[i],
            send_sem=own_send.at[i],
            recv_sem=own_sem.at[i],
            device_id=swapped,
            device_id_type=MESH,
        )

    def own_wait(i):
        @pl.when(stays)
        def _():
            own_local(i).wait()

        @pl.when(moves)
        def _():
            own_remote(i, own).wait_recv()

    def patch_load():
        return pltpu.make_async_copy(patches_in, pat, pat_sem.at[0])

    @pl.when(stays)
    def _():
        for i in range(5):
            own_local(i).start()

    @pl.when(section == 0)
    def _():
        patch_load().start()

    barrier = pltpu.get_barrier_semaphore()

    def greet(partner):
        pl.semaphore_signal(barrier, inc=1, device_id=partner, device_id_type=MESH)

    for partner in (up, down, sibling, after, before):
        greet(partner)

    @pl.when(r + k > 0)
    def _():
        greet(last_to)

    @pl.when(r + 1 - k > 0)
    def _():
        greet(last_from)

    @pl.when(moves)
    def _():
        greet(swapped)

    pl.semaphore_wait(barrier, 6 + r + lax.rem(r + k, 2))

    @pl.when(moves)
    def _():
        for i in range(5):
            own_remote(i, 2 * z + r).start()

    def hops(way, piece):
        return half if (piece == W_OUT) == (way == 1) else half - 1

    def ring(way, hop, piece, arriving):
        distance = hop + 1 if arriving else hop
        place = lax.rem(z + (zn - distance if way == 0 else distance), zn)
        ref = slot_ref(piece, 2 * place + k)
        return pltpu.make_async_remote_copy(
            src_ref=ref,
            dst_ref=ref,
            send_sem=ring_send.at[way, hop, piece],
            recv_sem=ring_recv.at[way, hop, piece],
            device_id=up if way == 0 else down,
            device_id_type=MESH,
        )

    def across(offset, piece, arriving):
        place = lax.rem(z + offset, zn)
        ref = slot_ref(piece, 2 * place + (1 - k if arriving else k))
        return pltpu.make_async_remote_copy(
            src_ref=ref,
            dst_ref=ref,
            send_sem=core_send.at[offset, piece],
            recv_sem=core_recv.at[offset, piece],
            device_id=sibling,
            device_id_type=MESH,
        )

    for piece in (BIAS, W_IN, W_OUT):
        own_wait(piece)
        ring(0, 0, piece, False).start()
        ring(1, 0, piece, False).start()
        across(0, piece, False).start()

    own_wait(3)
    own_wait(4)
    gain_row = small[1:2, 128:]
    shift_row = small[2:3, 128:]
    out_row = small[0:1, 128:]
    normed, widened = normalize(x0[...], gain_row, shift_row)
    normed0[...] = normed
    acc[...] = widened + out_row

    def add_shard(slot):
        at = pl.ds(pl.multiple_of(slot * shard, shard), shard)
        preact = rows_times(normed0[...], win[at, :]) + bias[slot][0:1, :shard]
        hidden = activate(preact).astype(jnp.bfloat16)
        acc[...] += jnp.dot(hidden, wout[at, :], preferred_element_type=jnp.float32)

    def add_offset(offset):
        for piece in (BIAS, W_IN, W_OUT):
            across(offset, piece, True).wait_recv()
        place = lax.rem(z + offset, zn)
        add_shard(2 * place)
        add_shard(2 * place + 1)

    def take(hop, piece):
        for way in (0, 1):
            if hop < hops(way, piece):
                ring(way, hop, piece, True).wait_recv()
                if hop + 1 < hops(way, piece):
                    ring(way, hop + 1, piece, False).start()
                across((zn - hop - 1 if way == 0 else hop + 1) % zn, piece, False).start()

    def select_send():
        return pltpu.make_async_remote_copy(
            src_ref=sel,
            dst_ref=sel_far,
            send_sem=sel_send.at[0],
            recv_sem=sel_recv.at[0],
            device_id=swapped,
            device_id_type=MESH,
        )

    for hop in range(half):
        take(hop, BIAS)
        take(hop, W_IN)
        add_offset((zn - hop) % zn)
        take(hop, W_OUT)
        if hop:
            add_offset(hop)
        else:

            @pl.when(section == 0)
            def _():
                patch_load().wait()
                for i in range(TICKS - 1):
                    sel[i] = pat[plan[i]]

            @pl.when((section == 0) & (r == 1))
            def _():
                select_send().start()

    add_offset(half)

    @pl.when((section == 1) & (r == 0))
    def _():
        select_send().wait_recv()

    for first in range(0, 2 * zn, 4):
        bias_row[0:1, pl.ds(first * shard, 4 * shard)] = jnp.concatenate(
            [bias[slot][0:1, :shard] for slot in range(first, first + 4)], axis=1
        )

    def chunk_rows(chunk):
        return pl.ds(chunk * rows, rows)

    def hop_on(tick, chunk):
        at = chunk_rows(chunk)
        return pltpu.make_async_remote_copy(
            src_ref=prod.at[tick, at],
            dst_ref=arr.at[tick, at],
            send_sem=hop_send.at[tick, chunk],
            recv_sem=hop_recv.at[tick, chunk],
            device_id=after,
            device_id_type=MESH,
        )

    def hop_last(chunk):
        at = chunk_rows(chunk)
        return pltpu.make_async_remote_copy(
            src_ref=prod.at[TICKS - 1, at],
            dst_ref=out.at[0, TICKS - 1, at],
            send_sem=hop_send.at[TICKS - 1, chunk],
            recv_sem=hop_recv.at[TICKS - 1, chunk],
            device_id=last_to,
            device_id_type=MESH,
        )

    def record_local(tick, chunk):
        at = chunk_rows(chunk)
        return pltpu.make_async_copy(
            arr.at[tick, at], out.at[0, tick, at], back_recv.at[tick, chunk]
        )

    def record_remote(tick, chunk):
        at = chunk_rows(chunk)
        return pltpu.make_async_remote_copy(
            src_ref=arr.at[tick, at],
            dst_ref=out.at[0, tick, at],
            send_sem=back_send.at[tick, chunk],
            recv_sem=back_recv.at[tick, chunk],
            device_id=swapped,
            device_id_type=MESH,
        )

    prod[0] = acc[...].astype(jnp.bfloat16)
    for chunk in range(CHUNKS):
        hop_on(0, chunk).start()

    wide = 256

    def step(tick, chunk):
        at = chunk_rows(chunk)
        hop_on(tick - 1, chunk).wait_recv()

        @pl.when(stays)
        def _():
            record_local(tick - 1, chunk).start()

        @pl.when(moves)
        def _():
            record_remote(tick - 1, chunk).start()

        cur[...] = arr[tick - 1, at, :]

        @pl.when((section == 0) & (r == 0))
        def _():
            cur[...] = sel[tick - 1, at, :]

        @pl.when((section == 1) & (r == 0))
        def _():
            cur[...] = sel_far[tick - 1, at, :]

        normed, widened = normalize(cur[...], gain_row, shift_row)
        for low in range(0, width, wide):
            preact = rows_times(normed, win[low : low + wide, :]) + bias_row[0:1, low : low + wide]
            hid[:, low : low + wide] = activate(preact).astype(jnp.bfloat16)
        for low in range(0, depth, wide):
            mixed = jnp.dot(
                hid[...], wout[:, low : low + wide], preferred_element_type=jnp.float32
            )
            prod[tick, at, low : low + wide] = (
                widened[:, low : low + wide] + mixed + out_row[:, low : low + wide]
            ).astype(jnp.bfloat16)

        @pl.when(tick < TICKS - 1)
        def _():
            hop_on(tick, chunk).start()

        @pl.when(tick == TICKS - 1)
        def _():
            hop_last(chunk).start()

    @pl.loop(1, TICKS)
    def _(tick):
        for chunk in range(CHUNKS):
            step(tick, chunk)

    for tick in range(TICKS - 1):
        for chunk in range(CHUNKS):

            @pl.when(stays)
            def _():
                record_local(tick, chunk).wait()

            @pl.when(moves)
            def _():
                record_remote(tick, chunk).wait_recv()
                record_remote(tick, chunk).wait_send()

            hop_on(tick, chunk).wait_send()

    @pl.when(moves)
    def _():
        for i in range(5):
            own_remote(i, 2 * z + r).wait_send()

    @pl.when((section == 0) & (r == 1))
    def _():
        select_send().wait_send()

    for piece in (BIAS, W_IN, W_OUT):
        for way in (0, 1):
            for hop in range(hops(way, piece)):
                ring(way, hop, piece, False).wait_send()
        for offset in range(zn):
            across(offset, piece, False).wait_send()
    for chunk in range(CHUNKS):
        hop_last(chunk).wait_send()
        hop_last(chunk).wait_recv()


def shards(
    section_inputs, w_in, in_bias, w_out, out_bias, norm_gain, norm_bias, patches, plan, *, yn, zn
):
    tokens, depth = section_inputs.shape[1:]
    shard = w_in.shape[1]
    width = 2 * zn * shard
    lanes = -shard % 128
    small = jnp.concatenate(
        [
            jnp.pad(in_bias.astype(jnp.float32), ((0, 7), (0, lanes))),
            jnp.pad(jnp.concatenate([out_bias, norm_gain, norm_bias]), ((0, 5), (0, 0))),
        ],
        axis=1,
    )
    anywhere = pl.BlockSpec(memory_space=pl.ANY)
    half = zn // 2
    dma = pltpu.SemaphoreType.DMA
    return pl.pallas_call(
        functools.partial(block_kernel, yn, zn),
        out_shape=jax.ShapeDtypeStruct((1, TICKS, tokens, depth), jnp.bfloat16),
        in_specs=[anywhere] * 5 + [pl.BlockSpec(memory_space=pltpu.SMEM)],
        out_specs=anywhere,
        scratch_shapes=[
            pltpu.VMEM((tokens, depth), jnp.bfloat16),
            pltpu.VMEM((width, depth), jnp.bfloat16),
            pltpu.VMEM((width, depth), jnp.bfloat16),
            pltpu.VMEM(small.shape, jnp.float32),
            pltpu.VMEM((2 * zn, 8, 128), jnp.float32),
            pltpu.VMEM((8, width), jnp.float32),
            pltpu.VMEM(patches.shape, jnp.bfloat16),
            pltpu.VMEM((TICKS - 1, tokens, depth), jnp.bfloat16),
            pltpu.VMEM((TICKS - 1, tokens, depth), jnp.bfloat16),
            pltpu.VMEM((tokens // CHUNKS, depth), jnp.bfloat16),
            pltpu.VMEM((tokens, depth), jnp.bfloat16),
            pltpu.VMEM((tokens, depth), jnp.float32),
            pltpu.VMEM((tokens // CHUNKS, width), jnp.bfloat16),
            pltpu.VMEM((TICKS, tokens, depth), jnp.bfloat16),
            pltpu.VMEM((TICKS - 1, tokens, depth), jnp.bfloat16),
            dma((5,)),
            dma((5,)),
            dma((2, half, 3)),
            dma((2, half, 3)),
            dma((2 * half, 3)),
            dma((2 * half, 3)),
            dma((1,)),
            dma((1,)),
            dma((1,)),
            dma((TICKS, CHUNKS)),
            dma((TICKS, CHUNKS)),
            dma((TICKS - 1, CHUNKS)),
            dma((TICKS - 1, CHUNKS)),
        ],
        compiler_params=pltpu.CompilerParams(collective_id=0, has_side_effects=True),
    )(section_inputs, w_in, w_out, small, patches, plan)


def solution(mesh):
    placed = (
        P("section", "tensor", None),
        P("section", "tensor", None),
        P("section", "tensor"),
        P("section", "tensor", None),
        P("section", None),
        P("section", None),
        P("section", None),
        P(None, "tensor", None),
        P(),
    )
    return jax.shard_map(
        functools.partial(
            shards, yn=mesh.shape["section"] // 2, zn=mesh.shape["tensor"] // 2
        ),
        mesh=mesh,
        in_specs=placed,
        out_specs=P("section", None, "tensor", None),
        check_vma=False,
    )
```

```python
import functools

import jax
import jax.numpy as jnp
from jax import lax
from jax.experimental import pallas as pl
from jax.experimental.pallas import tpu as pltpu
from jax.sharding import PartitionSpec as P

TICKS = 4
CHUNKS = 2
MESH = pl.DeviceIdType.MESH

norm_floor = 0.1
gelu_slope = 1.702

PIECES = 5


def normalize(current, gain_row, shift_row):
    widened = current.astype(jnp.float32)
    average = jnp.mean(widened, axis=-1, keepdims=True)
    centered = widened - average
    variance = jnp.mean(centered * centered, axis=-1, keepdims=True)
    normed = (centered * lax.rsqrt(variance + norm_floor) * gain_row + shift_row).astype(
        jnp.bfloat16
    )
    return (normed, widened)


def activate(preact):
    return preact * jax.nn.sigmoid(gelu_slope * preact)


def rows_times(normed, rows):
    return lax.dot_general(
        normed, rows, (((1,), (1,)), ((), ())), preferred_element_type=jnp.float32
    )


def block_kernel(
    yn, zn,
    x_in, w_in, w_out, small_in, patches_in, plan, out,
    x0, win, wout, small, bias, bias_row, pat, sel, sel_far, cur, normed0, acc, hid, prod, arr,
    own_sem, own_send, ring_send, ring_recv, core_send, core_recv,
    pat_sem, sel_send, sel_recv, hop_send, hop_recv, back_send, back_recv,
):
    section = lax.axis_index("section")
    tensor = lax.axis_index("tensor")
    k = lax.rem(section, 2)
    y = lax.div(section, 2)
    r = lax.rem(tensor, 2)
    z = lax.div(tensor, 2)
    tokens, depth = x0.shape
    shard = w_in.shape[1]
    width = win.shape[0]
    half = zn // 2
    rows = tokens // CHUNKS

    def device(y, k, z, r):
        return (2 * y + k, 2 * z + r)

    up = device(y, k, lax.rem(z + 1, zn), r)
    down = device(y, k, lax.rem(z + zn - 1, zn), r)
    onward = device(y, k, lax.rem(z + 1 + k * (zn - 2), zn), r)
    sibling = device(y, 1 - k, z, r)
    swapped = device(y, r, z, k)
    after = device(lax.rem(y + r, yn), k, z, 1 - r)
    before = device(lax.rem(y + yn - 1 + r, yn), k, z, 1 - r)
    last_to = device(lax.rem(y + r, yn), 1 - r, z, k)
    last_from = device(lax.rem(y + yn - 1 + k, yn), r, z, 1 - k)
    stays = r == k
    moves = r != k

    part = shard // 2

    def slot_ref(piece, slot):
        if piece == 0:
            return bias.at[slot]
        whole = win if piece < 3 else wout
        first = slot * shard + (piece + 1) % 2 * part
        return whole.at[pl.ds(pl.multiple_of(first, part), part)]

    own = 2 * z + k
    sources = (
        small_in.at[:, pl.ds(0, 128)],
        w_in.at[0, pl.ds(0, part)],
        w_in.at[0, pl.ds(part, part)],
        w_out.at[0, pl.ds(0, part)],
        w_out.at[0, pl.ds(part, part)],
        small_in,
        x_in.at[0],
    )

    def own_targets(slot):
        return tuple(slot_ref(piece, slot) for piece in range(PIECES)) + (small, x0)

    def own_local(i):
        return pltpu.make_async_copy(sources[i], own_targets(own)[i], own_sem.at[i])

    def own_remote(i, slot):
        return pltpu.make_async_remote_copy(
            src_ref=sources[i],
            dst_ref=own_targets(slot)[i],
            send_sem=own_send.at[i],
            recv_sem=own_sem.at[i],
            device_id=swapped,
            device_id_type=MESH,
        )

    def own_wait(i):
        @pl.when(stays)
        def _():
            own_local(i).wait()

        @pl.when(moves)
        def _():
            own_remote(i, own).wait_recv()

    def patch_load():
        return pltpu.make_async_copy(patches_in, pat, pat_sem.at[0])

    @pl.when(stays)
    def _():
        for i in range(PIECES + 2):
            own_local(i).start()

    @pl.when(section == 0)
    def _():
        patch_load().start()

    barrier = pltpu.get_barrier_semaphore()

    def greet(partner):
        pl.semaphore_signal(barrier, inc=1, device_id=partner, device_id_type=MESH)

    for partner in (up, down, sibling, after, before):
        greet(partner)

    @pl.when(r + k > 0)
    def _():
        greet(last_to)

    @pl.when(r + 1 - k > 0)
    def _():
        greet(last_from)

    @pl.when(moves)
    def _():
        greet(swapped)

    pl.semaphore_wait(barrier, 6 + r + lax.rem(r + k, 2))

    @pl.when(moves)
    def _():
        for i in range(PIECES + 2):
            own_remote(i, 2 * z + r).start()

    first_stream = (r, 1 - r)

    def place_at(distance):
        return lax.rem(z + lax.rem(k * 2 * distance + zn - distance, zn), zn)

    def ring(hop, i, piece, arriving):
        ref = slot_ref(piece, 2 * place_at(hop + 1 if arriving else hop) + first_stream[i])
        return pltpu.make_async_remote_copy(
            src_ref=ref,
            dst_ref=ref,
            send_sem=ring_send.at[hop, i, piece],
            recv_sem=ring_recv.at[hop, i, piece],
            device_id=onward,
            device_id_type=MESH,
        )

    def across(distance, i, piece, arriving):
        place = place_at((zn - distance) % zn if arriving else distance)
        ref = slot_ref(piece, 2 * place + first_stream[i])
        return pltpu.make_async_remote_copy(
            src_ref=ref,
            dst_ref=ref,
            send_sem=core_send.at[distance, i, piece],
            recv_sem=core_recv.at[distance, i, piece],
            device_id=sibling,
            device_id_type=MESH,
        )

    def farthest(arriving):
        return [(k == (1 if arriving else 0), range(0, 3)), (k == (0 if arriving else 1), range(3, 5))]

    for i, mine in ((0, stays), (1, moves)):
        for piece in range(PIECES):

            @pl.when(mine)
            def _():
                own_wait(piece)
                across(0, i, piece, False).start()

            @pl.when(jnp.logical_not(mine))
            def _():
                across(0, i, piece, True).wait_recv()

            ring(0, i, piece, False).start()

    own_wait(PIECES)
    own_wait(PIECES + 1)
    gain_row = small[1:2, 128:]
    shift_row = small[2:3, 128:]
    out_row = small[0:1, 128:]
    normed, widened = normalize(x0[...], gain_row, shift_row)
    normed0[...] = normed
    acc[...] = widened + out_row

    def add_place(place):
        at = pl.ds(pl.multiple_of(place * 2 * shard, 2 * shard), 2 * shard)
        both = jnp.concatenate(
            [bias[2 * place][0:1, :shard], bias[2 * place + 1][0:1, :shard]], axis=1
        )
        hidden = activate(rows_times(normed0[...], win[at, :]) + both).astype(jnp.bfloat16)
        acc[...] += jnp.dot(hidden, wout[at, :], preferred_element_type=jnp.float32)

    def take(hop):
        for i in (0, 1):
            for piece in range(PIECES):
                ring(hop, i, piece, True).wait_recv()
                if hop + 2 < half:
                    ring(hop + 1, i, piece, False).start()
                across(hop + 1, i, piece, False).start()
            if hop + 2 == half:
                for here, pieces in farthest(False):

                    @pl.when(here)
                    def _():
                        for piece in pieces:
                            ring(hop + 1, i, piece, False).start()

    def take_farthest():
        for here, pieces in farthest(False):

            @pl.when(here)
            def _():
                for i in (0, 1):
                    for piece in pieces:
                        ring(half - 1, i, piece, True).wait_recv()
                        across(half, i, piece, False).start()

    def given(distance):
        for i in (0, 1):
            for piece in range(PIECES):
                across(distance, i, piece, True).wait_recv()

    def given_farthest():
        for here, pieces in farthest(True):

            @pl.when(here)
            def _():
                for i in (0, 1):
                    for piece in pieces:
                        across(half, i, piece, True).wait_recv()

    def select_send():
        return pltpu.make_async_remote_copy(
            src_ref=sel,
            dst_ref=sel_far,
            send_sem=sel_send.at[0],
            recv_sem=sel_recv.at[0],
            device_id=swapped,
            device_id_type=MESH,
        )

    add_place(z)
    for hop in range(half - 1):
        take(hop)
        add_place(place_at(hop + 1))
        if hop == 1:

            @pl.when(section == 0)
            def _():
                patch_load().wait()
                for i in range(TICKS - 1):
                    sel[i] = pat[plan[i]]

            @pl.when((section == 0) & (r == 1))
            def _():
                select_send().start()

        if hop >= 2:
            given(hop - 1)
            add_place(place_at(zn - hop + 1))
    for distance in range(max(1, half - 2), half):
        given(distance)
        add_place(place_at(zn - distance))
    take_farthest()
    given_farthest()
    add_place(place_at(half))

    @pl.when((section == 1) & (r == 0))
    def _():
        select_send().wait_recv()

    for first in range(0, 2 * zn, 4):
        bias_row[0:1, pl.ds(first * shard, 4 * shard)] = jnp.concatenate(
            [bias[slot][0:1, :shard] for slot in range(first, first + 4)], axis=1
        )

    def chunk_rows(chunk):
        return pl.ds(chunk * rows, rows)

    def hop_on(tick, chunk):
        at = chunk_rows(chunk)
        return pltpu.make_async_remote_copy(
            src_ref=prod.at[tick, at],
            dst_ref=arr.at[tick, at],
            send_sem=hop_send.at[tick, chunk],
            recv_sem=hop_recv.at[tick, chunk],
            device_id=after,
            device_id_type=MESH,
        )

    def hop_last(chunk):
        at = chunk_rows(chunk)
        return pltpu.make_async_remote_copy(
            src_ref=prod.at[TICKS - 1, at],
            dst_ref=out.at[0, TICKS - 1, at],
            send_sem=hop_send.at[TICKS - 1, chunk],
            recv_sem=hop_recv.at[TICKS - 1, chunk],
            device_id=last_to,
            device_id_type=MESH,
        )

    def record_local(tick, chunk):
        at = chunk_rows(chunk)
        return pltpu.make_async_copy(
            arr.at[tick, at], out.at[0, tick, at], back_recv.at[tick, chunk]
        )

    def record_remote(tick, chunk):
        at = chunk_rows(chunk)
        return pltpu.make_async_remote_copy(
            src_ref=arr.at[tick, at],
            dst_ref=out.at[0, tick, at],
            send_sem=back_send.at[tick, chunk],
            recv_sem=back_recv.at[tick, chunk],
            device_id=swapped,
            device_id_type=MESH,
        )

    prod[0] = acc[...].astype(jnp.bfloat16)
    for chunk in range(CHUNKS):
        hop_on(0, chunk).start()

    wide = 256

    def step(tick, chunk):
        at = chunk_rows(chunk)
        hop_on(tick - 1, chunk).wait_recv()

        @pl.when(stays)
        def _():
            record_local(tick - 1, chunk).start()

        @pl.when(moves)
        def _():
            record_remote(tick - 1, chunk).start()

        cur[...] = arr[tick - 1, at, :]

        @pl.when((section == 0) & (r == 0))
        def _():
            cur[...] = sel[tick - 1, at, :]

        @pl.when((section == 1) & (r == 0))
        def _():
            cur[...] = sel_far[tick - 1, at, :]

        normed, widened = normalize(cur[...], gain_row, shift_row)
        for low in range(0, width, wide):
            preact = rows_times(normed, win[low : low + wide, :]) + bias_row[0:1, low : low + wide]
            hid[:, low : low + wide] = activate(preact).astype(jnp.bfloat16)
        for low in range(0, depth, wide):
            mixed = jnp.dot(
                hid[...], wout[:, low : low + wide], preferred_element_type=jnp.float32
            )
            prod[tick, at, low : low + wide] = (
                widened[:, low : low + wide] + mixed + out_row[:, low : low + wide]
            ).astype(jnp.bfloat16)

        @pl.when(tick < TICKS - 1)
        def _():
            hop_on(tick, chunk).start()

        @pl.when(tick == TICKS - 1)
        def _():
            hop_last(chunk).start()

    @pl.loop(1, TICKS)
    def _(tick):
        for chunk in range(CHUNKS):
            step(tick, chunk)

    for tick in range(TICKS - 1):
        for chunk in range(CHUNKS):

            @pl.when(stays)
            def _():
                record_local(tick, chunk).wait()

            @pl.when(moves)
            def _():
                record_remote(tick, chunk).wait_recv()
                record_remote(tick, chunk).wait_send()

            hop_on(tick, chunk).wait_send()

    @pl.when(moves)
    def _():
        for i in range(PIECES + 2):
            own_remote(i, 2 * z + r).wait_send()

    @pl.when((section == 0) & (r == 1))
    def _():
        select_send().wait_send()

    for i, mine in ((0, stays), (1, moves)):
        for piece in range(PIECES):

            @pl.when(mine)
            def _():
                across(0, i, piece, False).wait_send()

            for hop in range(half - 1):
                ring(hop, i, piece, False).wait_send()
                across(hop + 1, i, piece, False).wait_send()
        for here, pieces in farthest(False):

            @pl.when(here)
            def _():
                for piece in pieces:
                    ring(half - 1, i, piece, False).wait_send()
                    across(half, i, piece, False).wait_send()

    for chunk in range(CHUNKS):
        hop_last(chunk).wait_send()
        hop_last(chunk).wait_recv()


def shards(
    section_inputs, w_in, in_bias, w_out, out_bias, norm_gain, norm_bias, patches, plan, *, yn, zn
):
    tokens, depth = section_inputs.shape[1:]
    shard = w_in.shape[1]
    width = 2 * zn * shard
    lanes = -shard % 128
    small = jnp.concatenate(
        [
            jnp.pad(in_bias.astype(jnp.float32), ((0, 7), (0, lanes))),
            jnp.pad(jnp.concatenate([out_bias, norm_gain, norm_bias]), ((0, 5), (0, 0))),
        ],
        axis=1,
    )
    anywhere = pl.BlockSpec(memory_space=pl.ANY)
    half = zn // 2
    dma = pltpu.SemaphoreType.DMA
    return pl.pallas_call(
        functools.partial(block_kernel, yn, zn),
        out_shape=jax.ShapeDtypeStruct((1, TICKS, tokens, depth), jnp.bfloat16),
        in_specs=[anywhere] * 5 + [pl.BlockSpec(memory_space=pltpu.SMEM)],
        out_specs=anywhere,
        scratch_shapes=[
            pltpu.VMEM((tokens, depth), jnp.bfloat16),
            pltpu.VMEM((width, depth), jnp.bfloat16),
            pltpu.VMEM((width, depth), jnp.bfloat16),
            pltpu.VMEM(small.shape, jnp.float32),
            pltpu.VMEM((2 * zn, 8, 128), jnp.float32),
            pltpu.VMEM((8, width), jnp.float32),
            pltpu.VMEM(patches.shape, jnp.bfloat16),
            pltpu.VMEM((TICKS - 1, tokens, depth), jnp.bfloat16),
            pltpu.VMEM((TICKS - 1, tokens, depth), jnp.bfloat16),
            pltpu.VMEM((tokens // CHUNKS, depth), jnp.bfloat16),
            pltpu.VMEM((tokens, depth), jnp.bfloat16),
            pltpu.VMEM((tokens, depth), jnp.float32),
            pltpu.VMEM((tokens // CHUNKS, width), jnp.bfloat16),
            pltpu.VMEM((TICKS, tokens, depth), jnp.bfloat16),
            pltpu.VMEM((TICKS - 1, tokens, depth), jnp.bfloat16),
            dma((PIECES + 2,)),
            dma((PIECES + 2,)),
            dma((half, 2, PIECES)),
            dma((half, 2, PIECES)),
            dma((half + 1, 2, PIECES)),
            dma((half + 1, 2, PIECES)),
            dma((1,)),
            dma((1,)),
            dma((1,)),
            dma((TICKS, CHUNKS)),
            dma((TICKS, CHUNKS)),
            dma((TICKS - 1, CHUNKS)),
            dma((TICKS - 1, CHUNKS)),
        ],
        compiler_params=pltpu.CompilerParams(collective_id=0, has_side_effects=True),
    )(section_inputs, w_in, w_out, small, patches, plan)


def solution(mesh):
    placed = (
        P("section", "tensor", None),
        P("section", "tensor", None),
        P("section", "tensor"),
        P("section", "tensor", None),
        P("section", None),
        P("section", None),
        P("section", None),
        P(None, "tensor", None),
        P(),
    )
    return jax.shard_map(
        functools.partial(
            shards, yn=mesh.shape["section"] // 2, zn=mesh.shape["tensor"] // 2
        ),
        mesh=mesh,
        in_specs=placed,
        out_specs=P("section", None, "tensor", None),
        check_vma=False,
    )
```

```python
import functools

import jax
import jax.numpy as jnp
from jax import lax
from jax.experimental import pallas as pl
from jax.experimental.pallas import tpu as pltpu
from jax.sharding import PartitionSpec as P

TICKS = 4
CHUNKS = 2
MESH = pl.DeviceIdType.MESH

norm_floor = 0.1
gelu_slope = 1.702

OWN = 9
PIECES = 5


def normalize(current, gain_row, shift_row):
    widened = current.astype(jnp.float32)
    average = jnp.mean(widened, axis=-1, keepdims=True)
    centered = widened - average
    variance = jnp.mean(centered * centered, axis=-1, keepdims=True)
    normed = (centered * lax.rsqrt(variance + norm_floor) * gain_row + shift_row).astype(
        jnp.bfloat16
    )
    return (normed, widened)


def activate(preact):
    return preact * jax.nn.sigmoid(gelu_slope * preact)


def rows_times(normed, rows):
    return lax.dot_general(
        normed, rows, (((1,), (1,)), ((), ())), preferred_element_type=jnp.float32
    )


def block_kernel(
    yn, zn,
    x_in, w_in, w_out, bias_in, add_in, gain_in, shift_in, patches_in, plan, out,
    x0, win, wout, add, gain, shift, bias, bias_row, pat, sel, sel_far, cur, normed0, acc, hid, prod, arr,
    own_sem, own_send, ring_send, ring_recv, core_send, core_recv,
    pat_sem, sel_send, sel_recv, hop_send, hop_recv, record_send, record_recv,
):
    section = lax.axis_index("section")
    tensor = lax.axis_index("tensor")
    k = lax.rem(section, 2)
    y = lax.div(section, 2)
    r = lax.rem(tensor, 2)
    z = lax.div(tensor, 2)
    tokens, depth = x0.shape
    shard = w_in.shape[1]
    width = win.shape[0]
    near = (zn - 1) // 2
    rows = tokens // CHUNKS

    def device(y, k, z, r):
        return (2 * y + k, 2 * z + r)

    onward = device(y, k, lax.rem(z + 1 + k * (zn - 2), zn), r)
    inward = device(y, k, lax.rem(z + zn - 1 - k * (zn - 2), zn), r)
    sibling = device(y, 1 - k, z, r)
    swapped = device(y, r, z, k)
    after = device(lax.rem(y + r, yn), k, z, 1 - r)
    before = device(lax.rem(y + yn - 1 + r, yn), k, z, 1 - r)
    last_to = device(lax.rem(y + r, yn), 1 - r, z, k)
    last_from = device(lax.rem(y + yn - 1 + k, yn), r, z, 1 - k)
    stays = r == k
    moves = r != k

    part = shard // 2

    def slot_ref(piece, slot):
        if piece == 0:
            return bias.at[slot]
        whole = win if piece < 3 else wout
        first = slot * shard + (piece + 1) % 2 * part
        return whole.at[pl.ds(pl.multiple_of(first, part), part)]

    own = 2 * z + k
    sources = (
        bias_in,
        w_in.at[0, pl.ds(0, part)],
        w_in.at[0, pl.ds(part, part)],
        w_out.at[0, pl.ds(0, part)],
        w_out.at[0, pl.ds(part, part)],
        add_in,
        gain_in,
        shift_in,
        x_in.at[0],
    )

    def own_targets(slot):
        return tuple(slot_ref(piece, slot) for piece in range(PIECES)) + (
            add,
            gain,
            shift,
            x0,
        )

    def own_local(i):
        return pltpu.make_async_copy(sources[i], own_targets(own)[i], own_sem.at[i])

    def own_remote(i, slot):
        return pltpu.make_async_remote_copy(
            src_ref=sources[i],
            dst_ref=own_targets(slot)[i],
            send_sem=own_send.at[i],
            recv_sem=own_sem.at[i],
            device_id=swapped,
            device_id_type=MESH,
        )

    def own_wait(i):
        @pl.when(stays)
        def _():
            own_local(i).wait()

        @pl.when(moves)
        def _():
            own_remote(i, own).wait_recv()

    def patch_load():
        return pltpu.make_async_copy(patches_in, pat, pat_sem.at[0])

    @pl.when(stays)
    def _():
        for i in range(OWN):
            own_local(i).start()

    @pl.when(section == 0)
    def _():
        patch_load().start()

    barrier = pltpu.get_barrier_semaphore()

    def greet(partner):
        pl.semaphore_signal(barrier, inc=1, device_id=partner, device_id_type=MESH)

    for sender in (inward, sibling, before):
        greet(sender)

    @pl.when(moves)
    def _():
        greet(swapped)

    @pl.when((r == 1) & (k == 0))
    def _():
        greet(last_from)

    pl.semaphore_wait(barrier, 3 + r + k - r * k)

    @pl.when(moves)
    def _():
        for i in range(OWN):
            own_remote(i, 2 * z + r).start()

    first_stream = (r, 1 - r)

    def place_at(distance):
        return lax.rem(z + lax.rem(k * 2 * distance + zn - distance, zn), zn)

    def ring(hop, i, piece, arriving):
        ref = slot_ref(piece, 2 * place_at(hop + 1 if arriving else hop) + first_stream[i])
        return pltpu.make_async_remote_copy(
            src_ref=ref,
            dst_ref=ref,
            send_sem=ring_send.at[hop, i, piece],
            recv_sem=ring_recv.at[hop, i, piece],
            device_id=onward,
            device_id_type=MESH,
        )

    def across(distance, i, piece, arriving):
        place = place_at((zn - distance) % zn if arriving else distance)
        ref = slot_ref(piece, 2 * place + first_stream[i])
        return pltpu.make_async_remote_copy(
            src_ref=ref,
            dst_ref=ref,
            send_sem=core_send.at[distance, i, piece],
            recv_sem=core_recv.at[distance, i, piece],
            device_id=sibling,
            device_id_type=MESH,
        )

    for i, mine in ((0, stays), (1, moves)):
        for piece in range(PIECES):

            @pl.when(mine)
            def _():
                own_wait(piece)
                across(0, i, piece, False).start()

            @pl.when(jnp.logical_not(mine))
            def _():
                across(0, i, piece, True).wait_recv()

            ring(0, i, piece, False).start()

    for i in range(PIECES, OWN):
        own_wait(i)
    gain_row = gain[...]
    shift_row = shift[...]
    out_row = add[...]
    normed, widened = normalize(x0[...], gain_row, shift_row)
    normed0[...] = normed
    acc[...] = widened + out_row

    def add_rows(at, bias_here):
        preact = rows_times(normed0[...], win[at, :]) + bias_here
        hidden = activate(preact).astype(jnp.bfloat16)
        acc[...] += jnp.dot(hidden, wout[at, :], preferred_element_type=jnp.float32)

    def add_place(place):
        both = jnp.concatenate(
            [bias[2 * place][0:1, :shard], bias[2 * place + 1][0:1, :shard]], axis=1
        )
        add_rows(pl.ds(pl.multiple_of(place * 2 * shard, 2 * shard), 2 * shard), both)

    def add_stream(place, i):
        slot = 2 * place + first_stream[i]
        add_rows(pl.ds(pl.multiple_of(slot * shard, shard), shard), bias[slot][0:1, :shard])

    def take(hop):
        for i in (0, 1):
            for piece in range(PIECES):
                ring(hop, i, piece, True).wait_recv()
                if hop + 1 < near:
                    ring(hop + 1, i, piece, False).start()
                else:

                    @pl.when(k == 1)
                    def _():
                        ring(hop + 1, i, piece, False).start()

                across(hop + 1, i, piece, False).start()

    def given(distance):
        for i in (0, 1):
            for piece in range(PIECES):
                across(distance, i, piece, True).wait_recv()

    def select_send():
        return pltpu.make_async_remote_copy(
            src_ref=sel,
            dst_ref=sel_far,
            send_sem=sel_send.at[0],
            recv_sem=sel_recv.at[0],
            device_id=swapped,
            device_id_type=MESH,
        )

    add_place(z)
    for hop in range(near):
        take(hop)
        add_place(place_at(hop + 1))
        if hop == 1:

            @pl.when(section == 0)
            def _():
                patch_load().wait()
                for i in range(TICKS - 1):
                    sel[i] = pat[plan[i]]

            @pl.when((section == 0) & (r == 1))
            def _():
                select_send().start()

        if hop >= 2:
            given(hop - 1)
            add_place(place_at(zn - hop + 1))
    for distance in range(max(1, near - 1), near + 1):
        given(distance)
        add_place(place_at(zn - distance))
    for i in (0, 1):

        @pl.when(k == 1)
        def _():
            for piece in range(PIECES):
                ring(near, i, piece, True).wait_recv()
                across(near + 1, i, piece, False).start()

        @pl.when(k == 0)
        def _():
            for piece in range(PIECES):
                across(near + 1, i, piece, True).wait_recv()

        add_stream(place_at(near + 1), i)

    @pl.when((section == 1) & (r == 0))
    def _():
        select_send().wait_recv()

    for first in range(0, 2 * zn, 4):
        bias_row[0:1, pl.ds(first * shard, 4 * shard)] = jnp.concatenate(
            [bias[slot][0:1, :shard] for slot in range(first, first + 4)], axis=1
        )

    def chunk_rows(chunk):
        return pl.ds(chunk * rows, rows)

    def forward(tick, chunk, landing):
        at = chunk_rows(chunk)
        return pltpu.make_async_remote_copy(
            src_ref=prod.at[tick, at],
            dst_ref=landing.at[tick, at],
            send_sem=hop_send.at[tick, chunk],
            recv_sem=hop_recv.at[tick, chunk],
            device_id=after,
            device_id_type=MESH,
        )

    def record(tick, chunk):
        at = chunk_rows(chunk)
        return pltpu.make_async_remote_copy(
            src_ref=prod.at[tick, at],
            dst_ref=result.at[tick, at],
            send_sem=record_send.at[tick, chunk],
            recv_sem=record_recv.at[tick, chunk],
            device_id=last_to,
            device_id_type=MESH,
        )

    result = out.at[0]

    def send_on(tick, chunk):
        @pl.when(moves)
        def _():
            forward(tick, chunk, result).start()

        @pl.when(stays)
        def _():
            @pl.when(tick < TICKS - 1)
            def _():
                forward(tick, chunk, arr).start()

            record(tick, chunk).start()

    for chunk in range(CHUNKS):
        prod[0, chunk_rows(chunk)] = acc[chunk_rows(chunk), :].astype(jnp.bfloat16)
        send_on(0, chunk)

    wide = 256

    def step(tick, chunk):
        at = chunk_rows(chunk)

        @pl.when(stays)
        def _():
            forward(tick - 1, chunk, result).wait_recv()
            cur[...] = out[0, tick - 1, at, :]

        @pl.when(moves)
        def _():
            forward(tick - 1, chunk, arr).wait_recv()
            cur[...] = arr[tick - 1, at, :]

        @pl.when((section == 0) & (r == 0))
        def _():
            cur[...] = sel[tick - 1, at, :]

        @pl.when((section == 1) & (r == 0))
        def _():
            cur[...] = sel_far[tick - 1, at, :]

        normed, widened = normalize(cur[...], gain_row, shift_row)
        for low in range(0, width, wide):
            preact = rows_times(normed, win[low : low + wide, :]) + bias_row[0:1, low : low + wide]
            hid[:, low : low + wide] = activate(preact).astype(jnp.bfloat16)
        for low in range(0, depth, wide):
            mixed = jnp.dot(
                hid[...], wout[:, low : low + wide], preferred_element_type=jnp.float32
            )
            prod[tick, at, low : low + wide] = (
                widened[:, low : low + wide] + mixed + out_row[:, low : low + wide]
            ).astype(jnp.bfloat16)

        send_on(tick, chunk)

    @pl.loop(1, TICKS)
    def _(tick):
        for chunk in range(CHUNKS):
            step(tick, chunk)

    @pl.when(moves)
    def _():
        for tick in range(TICKS):
            for chunk in range(CHUNKS):
                record(tick, chunk).wait_recv()
                forward(tick, chunk, result).wait_send()

    @pl.when(stays)
    def _():
        for tick in range(TICKS):
            for chunk in range(CHUNKS):
                if tick == TICKS - 1:
                    forward(tick, chunk, result).wait_recv()
                else:
                    forward(tick, chunk, arr).wait_send()
                record(tick, chunk).wait_send()

    @pl.when(moves)
    def _():
        for i in range(OWN):
            own_remote(i, 2 * z + r).wait_send()

    @pl.when((section == 0) & (r == 1))
    def _():
        select_send().wait_send()

    for i, mine in ((0, stays), (1, moves)):
        for piece in range(PIECES):

            @pl.when(mine)
            def _():
                across(0, i, piece, False).wait_send()

            for hop in range(near):
                ring(hop, i, piece, False).wait_send()
                across(hop + 1, i, piece, False).wait_send()

            @pl.when(k == 1)
            def _():
                ring(near, i, piece, False).wait_send()
                across(near + 1, i, piece, False).wait_send()


def shards(
    section_inputs, w_in, in_bias, w_out, out_bias, norm_gain, norm_bias, patches, plan, *, yn, zn
):
    tokens, depth = section_inputs.shape[1:]
    shard = w_in.shape[1]
    width = 2 * zn * shard
    bias_tile = jnp.pad(in_bias.astype(jnp.float32), ((0, 7), (0, -shard % 128)))
    anywhere = pl.BlockSpec(memory_space=pl.ANY)
    half = zn // 2
    dma = pltpu.SemaphoreType.DMA
    return pl.pallas_call(
        functools.partial(block_kernel, yn, zn),
        out_shape=pltpu.VMEM((1, TICKS, tokens, depth), jnp.bfloat16),
        in_specs=[anywhere] * 8 + [pl.BlockSpec(memory_space=pltpu.SMEM)],
        out_specs=pl.BlockSpec(memory_space=pltpu.VMEM),
        scratch_shapes=[
            pltpu.VMEM((tokens, depth), jnp.bfloat16),
            pltpu.VMEM((width, depth), jnp.bfloat16),
            pltpu.VMEM((width, depth), jnp.bfloat16),
            pltpu.VMEM((1, depth), jnp.float32),
            pltpu.VMEM((1, depth), jnp.float32),
            pltpu.VMEM((1, depth), jnp.float32),
            pltpu.VMEM((2 * zn, 8, 128), jnp.float32),
            pltpu.VMEM((8, width), jnp.float32),
            pltpu.VMEM(patches.shape, jnp.bfloat16),
            pltpu.VMEM((TICKS - 1, tokens, depth), jnp.bfloat16),
            pltpu.VMEM((TICKS - 1, tokens, depth), jnp.bfloat16),
            pltpu.VMEM((tokens // CHUNKS, depth), jnp.bfloat16),
            pltpu.VMEM((tokens, depth), jnp.bfloat16),
            pltpu.VMEM((tokens, depth), jnp.float32),
            pltpu.VMEM((tokens // CHUNKS, width), jnp.bfloat16),
            pltpu.VMEM((TICKS, tokens, depth), jnp.bfloat16),
            pltpu.VMEM((TICKS - 1, tokens, depth), jnp.bfloat16),
            dma((OWN,)),
            dma((OWN,)),
            dma((half, 2, PIECES)),
            dma((half, 2, PIECES)),
            dma((half + 1, 2, PIECES)),
            dma((half + 1, 2, PIECES)),
            dma((1,)),
            dma((1,)),
            dma((1,)),
            dma((TICKS, CHUNKS)),
            dma((TICKS, CHUNKS)),
            dma((TICKS, CHUNKS)),
            dma((TICKS, CHUNKS)),
        ],
        compiler_params=pltpu.CompilerParams(collective_id=0, has_side_effects=True),
    )(section_inputs, w_in, w_out, bias_tile, out_bias, norm_gain, norm_bias, patches, plan)


def solution(mesh):
    placed = (
        P("section", "tensor", None),
        P("section", "tensor", None),
        P("section", "tensor"),
        P("section", "tensor", None),
        P("section", None),
        P("section", None),
        P("section", None),
        P(None, "tensor", None),
        P(),
    )
    return jax.shard_map(
        functools.partial(
            shards, yn=mesh.shape["section"] // 2, zn=mesh.shape["tensor"] // 2
        ),
        mesh=mesh,
        in_specs=placed,
        out_specs=P("section", None, "tensor", None),
        check_vma=False,
    )
```

```python
import functools

import jax
import jax.numpy as jnp
from jax import lax
from jax.experimental import pallas as pl
from jax.experimental.pallas import tpu as pltpu
from jax.sharding import PartitionSpec as P

TICKS = 4
CHUNKS = 2
MESH = pl.DeviceIdType.MESH

norm_floor = 0.1
gelu_slope = 1.702

OWN = 7
PIECES = 3


def normalize(current, gain_row, shift_row):
    widened = current.astype(jnp.float32)
    average = jnp.mean(widened, axis=-1, keepdims=True)
    centered = widened - average
    variance = jnp.mean(centered * centered, axis=-1, keepdims=True)
    normed = (centered * lax.rsqrt(variance + norm_floor) * gain_row + shift_row).astype(
        jnp.bfloat16
    )
    return (normed, widened)


def activate(preact):
    return preact * jax.nn.sigmoid(gelu_slope * preact)


def rows_times(normed, rows):
    return lax.dot_general(
        normed, rows, (((1,), (1,)), ((), ())), preferred_element_type=jnp.float32
    )


def block_kernel(
    yn, zn,
    x_in, w_in, w_out, bias_in, add_in, gain_in, shift_in, patches_in, plan, out,
    x0, win, wout, add, gain, shift, bias, bias_row, pat, sel, sel_far, cur, normed0, acc, hid, prod, arr,
    own_sem, own_send, ring_send, ring_recv, core_send, core_recv,
    pat_sem, sel_send, sel_recv, hop_send, hop_recv, record_send, record_recv,
):
    section = lax.axis_index("section")
    tensor = lax.axis_index("tensor")
    k = lax.rem(section, 2)
    y = lax.div(section, 2)
    r = lax.rem(tensor, 2)
    z = lax.div(tensor, 2)
    tokens, depth = x0.shape
    shard = w_in.shape[1]
    width = win.shape[0]
    near = (zn - 1) // 2
    rows = tokens // CHUNKS

    def device(y, k, z, r):
        return (2 * y + k, 2 * z + r)

    onward = device(y, k, lax.rem(z + 1 + k * (zn - 2), zn), r)
    inward = device(y, k, lax.rem(z + zn - 1 - k * (zn - 2), zn), r)
    sibling = device(y, 1 - k, z, r)
    swapped = device(y, r, z, k)
    after = device(lax.rem(y + r, yn), k, z, 1 - r)
    before = device(lax.rem(y + yn - 1 + r, yn), k, z, 1 - r)
    last_to = device(lax.rem(y + r, yn), 1 - r, z, k)
    last_from = device(lax.rem(y + yn - 1 + k, yn), r, z, 1 - k)
    stays = r == k
    moves = r != k

    def slot_ref(piece, slot):
        if piece == 0:
            return bias.at[slot]
        whole = win if piece == 1 else wout
        return whole.at[pl.ds(pl.multiple_of(slot * shard, shard), shard)]

    own = 2 * z + k
    sources = (
        bias_in,
        w_in.at[0],
        w_out.at[0],
        add_in,
        gain_in,
        shift_in,
        x_in.at[0],
    )

    def own_targets(slot):
        return tuple(slot_ref(piece, slot) for piece in range(PIECES)) + (
            add,
            gain,
            shift,
            x0,
        )

    def own_local(i):
        return pltpu.make_async_copy(sources[i], own_targets(own)[i], own_sem.at[i])

    def own_remote(i, slot):
        return pltpu.make_async_remote_copy(
            src_ref=sources[i],
            dst_ref=own_targets(slot)[i],
            send_sem=own_send.at[i],
            recv_sem=own_sem.at[i],
            device_id=swapped,
            device_id_type=MESH,
        )

    def own_wait(i):
        @pl.when(stays)
        def _():
            own_local(i).wait()

        @pl.when(moves)
        def _():
            own_remote(i, own).wait_recv()

    def patch_load():
        return pltpu.make_async_copy(patches_in, pat, pat_sem.at[0])

    @pl.when(stays)
    def _():
        for i in range(OWN):
            own_local(i).start()

    @pl.when(section == 0)
    def _():
        patch_load().start()

    barrier = pltpu.get_barrier_semaphore()

    def greet(partner):
        pl.semaphore_signal(barrier, inc=1, device_id=partner, device_id_type=MESH)

    for sender in (inward, sibling, before):
        greet(sender)

    @pl.when(moves)
    def _():
        greet(swapped)

    @pl.when((r == 1) & (k == 0))
    def _():
        greet(last_from)

    pl.semaphore_wait(barrier, 3 + r + k - r * k)

    @pl.when(moves)
    def _():
        for i in range(OWN):
            own_remote(i, 2 * z + r).start()

    first_stream = (r, 1 - r)

    def place_at(distance):
        return lax.rem(z + lax.rem(k * 2 * distance + zn - distance, zn), zn)

    def ring(hop, i, piece, arriving):
        ref = slot_ref(piece, 2 * place_at(hop + 1 if arriving else hop) + first_stream[i])
        return pltpu.make_async_remote_copy(
            src_ref=ref,
            dst_ref=ref,
            send_sem=ring_send.at[hop, i, piece],
            recv_sem=ring_recv.at[hop, i, piece],
            device_id=onward,
            device_id_type=MESH,
        )

    def across(distance, i, piece, arriving):
        place = place_at((zn - distance) % zn if arriving else distance)
        ref = slot_ref(piece, 2 * place + first_stream[i])
        return pltpu.make_async_remote_copy(
            src_ref=ref,
            dst_ref=ref,
            send_sem=core_send.at[distance, i, piece],
            recv_sem=core_recv.at[distance, i, piece],
            device_id=sibling,
            device_id_type=MESH,
        )

    for i, mine in ((0, stays), (1, moves)):
        for piece in range(PIECES):

            @pl.when(mine)
            def _():
                own_wait(piece)
                across(0, i, piece, False).start()

            @pl.when(jnp.logical_not(mine))
            def _():
                across(0, i, piece, True).wait_recv()

            ring(0, i, piece, False).start()

    for i in range(PIECES, OWN):
        own_wait(i)
    gain_row = gain[...]
    shift_row = shift[...]
    out_row = add[...]
    normed, widened = normalize(x0[...], gain_row, shift_row)
    normed0[...] = normed
    acc[...] = widened + out_row

    def bias_of(slot):
        return bias[slot].astype(jnp.float32)

    def add_rows(at, bias_here):
        preact = rows_times(normed0[...], win[at, :]) + bias_here
        hidden = activate(preact).astype(jnp.bfloat16)
        acc[...] += jnp.dot(hidden, wout[at, :], preferred_element_type=jnp.float32)

    def add_place(place):
        both = jnp.concatenate(
            [bias_of(2 * place), bias_of(2 * place + 1)], axis=1
        )
        add_rows(pl.ds(pl.multiple_of(place * 2 * shard, 2 * shard), 2 * shard), both)

    def add_stream(place, i):
        slot = 2 * place + first_stream[i]
        add_rows(pl.ds(pl.multiple_of(slot * shard, shard), shard), bias_of(slot))

    def take(hop):
        for i in (0, 1):
            for piece in range(PIECES):
                ring(hop, i, piece, True).wait_recv()
                if hop + 1 < near:
                    ring(hop + 1, i, piece, False).start()
                else:

                    @pl.when(k == 1)
                    def _():
                        ring(hop + 1, i, piece, False).start()

                across(hop + 1, i, piece, False).start()

    def given(distance):
        for i in (0, 1):
            for piece in range(PIECES):
                across(distance, i, piece, True).wait_recv()

    def select_send():
        return pltpu.make_async_remote_copy(
            src_ref=sel,
            dst_ref=sel_far,
            send_sem=sel_send.at[0],
            recv_sem=sel_recv.at[0],
            device_id=swapped,
            device_id_type=MESH,
        )

    add_place(z)
    for hop in range(near):
        take(hop)
        add_place(place_at(hop + 1))
        if hop == 1:

            @pl.when(section == 0)
            def _():
                patch_load().wait()
                for i in range(TICKS - 1):
                    sel[i] = pat[plan[i]]

            @pl.when((section == 0) & (r == 1))
            def _():
                select_send().start()

        if hop >= 2:
            given(hop - 1)
            add_place(place_at(zn - hop + 1))
    for distance in range(max(1, near - 1), near + 1):
        given(distance)
        add_place(place_at(zn - distance))
    for i in (0, 1):

        @pl.when(k == 1)
        def _():
            for piece in range(PIECES):
                ring(near, i, piece, True).wait_recv()
                across(near + 1, i, piece, False).start()

        @pl.when(k == 0)
        def _():
            for piece in range(PIECES):
                across(near + 1, i, piece, True).wait_recv()

        add_stream(place_at(near + 1), i)

    @pl.when((section == 1) & (r == 0))
    def _():
        select_send().wait_recv()

    for first in range(0, 2 * zn, 4):
        bias_row[0:1, pl.ds(first * shard, 4 * shard)] = jnp.concatenate(
            [bias_of(slot) for slot in range(first, first + 4)], axis=1
        )

    def chunk_rows(chunk):
        return pl.ds(chunk * rows, rows)

    def forward(tick, chunk, landing):
        at = chunk_rows(chunk)
        return pltpu.make_async_remote_copy(
            src_ref=prod.at[tick, at],
            dst_ref=landing.at[tick, at],
            send_sem=hop_send.at[tick, chunk],
            recv_sem=hop_recv.at[tick, chunk],
            device_id=after,
            device_id_type=MESH,
        )

    def record(tick, chunk):
        at = chunk_rows(chunk)
        return pltpu.make_async_remote_copy(
            src_ref=prod.at[tick, at],
            dst_ref=result.at[tick, at],
            send_sem=record_send.at[tick, chunk],
            recv_sem=record_recv.at[tick, chunk],
            device_id=last_to,
            device_id_type=MESH,
        )

    result = out.at[0]

    def send_on(tick, chunk):
        @pl.when(moves)
        def _():
            forward(tick, chunk, result).start()

        @pl.when(stays)
        def _():
            @pl.when(tick < TICKS - 1)
            def _():
                forward(tick, chunk, arr).start()

            record(tick, chunk).start()

    for chunk in range(CHUNKS):
        prod[0, chunk_rows(chunk)] = acc[chunk_rows(chunk), :].astype(jnp.bfloat16)
        send_on(0, chunk)

    wide = 256

    def step(tick, chunk):
        at = chunk_rows(chunk)

        @pl.when(stays)
        def _():
            forward(tick - 1, chunk, result).wait_recv()
            cur[...] = out[0, tick - 1, at, :]

        @pl.when(moves)
        def _():
            forward(tick - 1, chunk, arr).wait_recv()
            cur[...] = arr[tick - 1, at, :]

        @pl.when((section == 0) & (r == 0))
        def _():
            cur[...] = sel[tick - 1, at, :]

        @pl.when((section == 1) & (r == 0))
        def _():
            cur[...] = sel_far[tick - 1, at, :]

        normed, widened = normalize(cur[...], gain_row, shift_row)
        for low in range(0, width, wide):
            preact = rows_times(normed, win[low : low + wide, :]) + bias_row[0:1, low : low + wide]
            hid[:, low : low + wide] = activate(preact).astype(jnp.bfloat16)
        for low in range(0, depth, wide):
            mixed = jnp.dot(
                hid[...], wout[:, low : low + wide], preferred_element_type=jnp.float32
            )
            prod[tick, at, low : low + wide] = (
                widened[:, low : low + wide] + mixed + out_row[:, low : low + wide]
            ).astype(jnp.bfloat16)

        send_on(tick, chunk)

    @pl.loop(1, TICKS)
    def _(tick):
        for chunk in range(CHUNKS):
            step(tick, chunk)

    @pl.when(moves)
    def _():
        for tick in range(TICKS):
            for chunk in range(CHUNKS):
                record(tick, chunk).wait_recv()
                forward(tick, chunk, result).wait_send()

    @pl.when(stays)
    def _():
        for tick in range(TICKS):
            for chunk in range(CHUNKS):
                if tick == TICKS - 1:
                    forward(tick, chunk, result).wait_recv()
                else:
                    forward(tick, chunk, arr).wait_send()
                record(tick, chunk).wait_send()

    @pl.when(moves)
    def _():
        for i in range(OWN):
            own_remote(i, 2 * z + r).wait_send()

    @pl.when((section == 0) & (r == 1))
    def _():
        select_send().wait_send()

    for i, mine in ((0, stays), (1, moves)):
        for piece in range(PIECES):

            @pl.when(mine)
            def _():
                across(0, i, piece, False).wait_send()

            for hop in range(near):
                ring(hop, i, piece, False).wait_send()
                across(hop + 1, i, piece, False).wait_send()

            @pl.when(k == 1)
            def _():
                ring(near, i, piece, False).wait_send()
                across(near + 1, i, piece, False).wait_send()


def shards(
    section_inputs, w_in, in_bias, w_out, out_bias, norm_gain, norm_bias, patches, plan, *, yn, zn
):
    tokens, depth = section_inputs.shape[1:]
    shard = w_in.shape[1]
    width = 2 * zn * shard
    anywhere = pl.BlockSpec(memory_space=pl.ANY)
    half = zn // 2
    dma = pltpu.SemaphoreType.DMA
    return pl.pallas_call(
        functools.partial(block_kernel, yn, zn),
        out_shape=pltpu.VMEM((1, TICKS, tokens, depth), jnp.bfloat16),
        in_specs=[anywhere] * 8 + [pl.BlockSpec(memory_space=pltpu.SMEM)],
        out_specs=pl.BlockSpec(memory_space=pltpu.VMEM),
        scratch_shapes=[
            pltpu.VMEM((tokens, depth), jnp.bfloat16),
            pltpu.VMEM((width, depth), jnp.bfloat16),
            pltpu.VMEM((width, depth), jnp.bfloat16),
            pltpu.VMEM((1, depth), jnp.float32),
            pltpu.VMEM((1, depth), jnp.float32),
            pltpu.VMEM((1, depth), jnp.float32),
            pltpu.VMEM((2 * zn, 1, shard), jnp.bfloat16),
            pltpu.VMEM((8, width), jnp.float32),
            pltpu.VMEM(patches.shape, jnp.bfloat16),
            pltpu.VMEM((TICKS - 1, tokens, depth), jnp.bfloat16),
            pltpu.VMEM((TICKS - 1, tokens, depth), jnp.bfloat16),
            pltpu.VMEM((tokens // CHUNKS, depth), jnp.bfloat16),
            pltpu.VMEM((tokens, depth), jnp.bfloat16),
            pltpu.VMEM((tokens, depth), jnp.float32),
            pltpu.VMEM((tokens // CHUNKS, width), jnp.bfloat16),
            pltpu.VMEM((TICKS, tokens, depth), jnp.bfloat16),
            pltpu.VMEM((TICKS - 1, tokens, depth), jnp.bfloat16),
            dma((OWN,)),
            dma((OWN,)),
            dma((half, 2, PIECES)),
            dma((half, 2, PIECES)),
            dma((half + 1, 2, PIECES)),
            dma((half + 1, 2, PIECES)),
            dma((1,)),
            dma((1,)),
            dma((1,)),
            dma((TICKS, CHUNKS)),
            dma((TICKS, CHUNKS)),
            dma((TICKS, CHUNKS)),
            dma((TICKS, CHUNKS)),
        ],
        compiler_params=pltpu.CompilerParams(collective_id=0, has_side_effects=True),
    )(section_inputs, w_in, w_out, in_bias, out_bias, norm_gain, norm_bias, patches, plan)


def solution(mesh):
    placed = (
        P("section", "tensor", None),
        P("section", "tensor", None),
        P("section", "tensor"),
        P("section", "tensor", None),
        P("section", None),
        P("section", None),
        P("section", None),
        P(None, "tensor", None),
        P(),
    )
    return jax.shard_map(
        functools.partial(
            shards, yn=mesh.shape["section"] // 2, zn=mesh.shape["tensor"] // 2
        ),
        mesh=mesh,
        in_specs=placed,
        out_specs=P("section", None, "tensor", None),
        check_vma=False,
    )
```

```python
import functools

import jax
import jax.numpy as jnp
from jax import lax
from jax.experimental import pallas as pl
from jax.experimental.pallas import tpu as pltpu
from jax.sharding import PartitionSpec as P

TICKS = 4
CHUNKS = 2
MESH = pl.DeviceIdType.MESH

norm_floor = 0.1
gelu_slope = 1.702

OWN = 7
PIECES = 3


def normalize(current, gain_row, shift_row):
    widened = current.astype(jnp.float32)
    average = jnp.mean(widened, axis=-1, keepdims=True)
    centered = widened - average
    variance = jnp.mean(centered * centered, axis=-1, keepdims=True)
    normed = (centered * lax.rsqrt(variance + norm_floor) * gain_row + shift_row).astype(
        jnp.bfloat16
    )
    return (normed, widened)


def activate(preact):
    return preact * jax.nn.sigmoid(gelu_slope * preact)


def rows_times(normed, rows):
    return lax.dot_general(
        normed, rows, (((1,), (1,)), ((), ())), preferred_element_type=jnp.float32
    )


def block_kernel(
    yn, zn,
    x_in, w_in, w_out, bias_in, add_in, gain_in, shift_in, patches_in, plan, out,
    x0, win, wout, add, gain, shift, bias, bias_row, pat, sel, sel_far, cur, normed0, acc, hid, prod, arr,
    own_sem, own_send, ring_send, ring_recv, core_send, core_recv,
    pat_sem, sel_send, sel_recv, hop_send, hop_recv, record_send, record_recv,
):
    section = lax.axis_index("section")
    tensor = lax.axis_index("tensor")
    k = lax.rem(section, 2)
    y = lax.div(section, 2)
    r = lax.rem(tensor, 2)
    z = lax.div(tensor, 2)
    tokens, depth = x0.shape
    shard = w_in.shape[1]
    width = win.shape[0]
    near = (zn - 1) // 2
    rows = tokens // CHUNKS

    def device(y, k, z, r):
        return (2 * y + k, 2 * z + r)

    onward = device(y, k, lax.rem(z + 1 + k * (zn - 2), zn), r)
    inward = device(y, k, lax.rem(z + zn - 1 - k * (zn - 2), zn), r)
    sibling = device(y, 1 - k, z, r)
    swapped = device(y, r, z, k)
    after = device(lax.rem(y + r, yn), k, z, 1 - r)
    before = device(lax.rem(y + yn - 1 + r, yn), k, z, 1 - r)
    last_to = device(lax.rem(y + r, yn), 1 - r, z, k)
    last_from = device(lax.rem(y + yn - 1 + k, yn), r, z, 1 - k)
    stays = r == k
    moves = r != k

    def slot_ref(piece, slot):
        if piece == 0:
            return bias.at[slot]
        whole = win if piece == 1 else wout
        return whole.at[pl.ds(pl.multiple_of(slot * shard, shard), shard)]

    own = 2 * z + k
    sources = (
        bias_in,
        w_in.at[0],
        w_out.at[0],
        add_in,
        gain_in,
        shift_in,
        x_in.at[0],
    )

    def own_targets(slot):
        return tuple(slot_ref(piece, slot) for piece in range(PIECES)) + (
            add,
            gain,
            shift,
            x0,
        )

    def own_local(i):
        return pltpu.make_async_copy(sources[i], own_targets(own)[i], own_sem.at[i])

    def own_remote(i, slot):
        return pltpu.make_async_remote_copy(
            src_ref=sources[i],
            dst_ref=own_targets(slot)[i],
            send_sem=own_send.at[i],
            recv_sem=own_sem.at[i],
            device_id=swapped,
            device_id_type=MESH,
        )

    def own_wait(i):
        @pl.when(stays)
        def _():
            own_local(i).wait()

        @pl.when(moves)
        def _():
            own_remote(i, own).wait_recv()

    def patch_load():
        return pltpu.make_async_copy(patches_in, pat, pat_sem.at[0])

    @pl.when(stays)
    def _():
        for i in range(OWN):
            own_local(i).start()

    @pl.when(section == 0)
    def _():
        patch_load().start()

    barrier = pltpu.get_barrier_semaphore()

    def greet(partner):
        pl.semaphore_signal(barrier, inc=1, device_id=partner, device_id_type=MESH)

    for sender in (inward, sibling, before):
        greet(sender)

    @pl.when(moves)
    def _():
        greet(swapped)

    @pl.when((r == 1) & (k == 0))
    def _():
        greet(last_from)

    pl.semaphore_wait(barrier, 3 + r + k - r * k)

    @pl.when(moves)
    def _():
        for i in range(OWN):
            own_remote(i, 2 * z + r).start()

    first_stream = (r, 1 - r)

    def place_at(distance):
        return lax.rem(z + lax.rem(k * 2 * distance + zn - distance, zn), zn)

    def ring(hop, i, piece, arriving):
        ref = slot_ref(piece, 2 * place_at(hop + 1 if arriving else hop) + first_stream[i])
        return pltpu.make_async_remote_copy(
            src_ref=ref,
            dst_ref=ref,
            send_sem=ring_send.at[hop, i, piece],
            recv_sem=ring_recv.at[hop, i, piece],
            device_id=onward,
            device_id_type=MESH,
        )

    def across(distance, i, piece, arriving):
        place = place_at((zn - distance) % zn if arriving else distance)
        ref = slot_ref(piece, 2 * place + first_stream[i])
        return pltpu.make_async_remote_copy(
            src_ref=ref,
            dst_ref=ref,
            send_sem=core_send.at[distance, i, piece],
            recv_sem=core_recv.at[distance, i, piece],
            device_id=sibling,
            device_id_type=MESH,
        )

    for i, mine in ((0, stays), (1, moves)):
        for piece in range(PIECES):

            @pl.when(mine)
            def _():
                own_wait(piece)
                across(0, i, piece, False).start()

            @pl.when(jnp.logical_not(mine))
            def _():
                across(0, i, piece, True).wait_recv()

            ring(0, i, piece, False).start()

    for i in range(PIECES, OWN):
        own_wait(i)
    gain_row = gain[...]
    shift_row = shift[...]
    out_row = add[...]
    normed, widened = normalize(x0[...], gain_row, shift_row)
    normed0[...] = normed
    acc[...] = widened + out_row

    def bias_of(slot):
        return bias[slot].astype(jnp.float32)

    def add_rows(at, bias_here):
        preact = rows_times(normed0[...], win[at, :]) + bias_here
        hidden = activate(preact).astype(jnp.bfloat16)
        acc[...] += jnp.dot(hidden, wout[at, :], preferred_element_type=jnp.float32)

    def add_place(place):
        both = jnp.concatenate(
            [bias_of(2 * place), bias_of(2 * place + 1)], axis=1
        )
        add_rows(pl.ds(pl.multiple_of(place * 2 * shard, 2 * shard), 2 * shard), both)

    def add_stream(place, i):
        slot = 2 * place + first_stream[i]
        add_rows(pl.ds(pl.multiple_of(slot * shard, shard), shard), bias_of(slot))

    def take(hop):
        for i in (0, 1):
            for piece in range(PIECES):
                ring(hop, i, piece, True).wait_recv()
                if hop + 1 < near:
                    ring(hop + 1, i, piece, False).start()
                else:

                    @pl.when(k == 1)
                    def _():
                        ring(hop + 1, i, piece, False).start()

                across(hop + 1, i, piece, False).start()

    def given(distance):
        for i in (0, 1):
            for piece in range(PIECES):
                across(distance, i, piece, True).wait_recv()

    def select_send():
        return pltpu.make_async_remote_copy(
            src_ref=sel,
            dst_ref=sel_far,
            send_sem=sel_send.at[0],
            recv_sem=sel_recv.at[0],
            device_id=swapped,
            device_id_type=MESH,
        )

    add_place(z)
    for hop in range(near):
        take(hop)
        add_place(place_at(hop + 1))
        if hop == 1:

            @pl.when(section == 0)
            def _():
                patch_load().wait()
                for i in range(TICKS - 1):
                    sel[i] = pat[plan[i]]

            @pl.when((section == 0) & (r == 1))
            def _():
                select_send().start()

        if hop >= 2:
            given(hop - 1)
            add_place(place_at(zn - hop + 1))
    for distance in range(max(1, near - 1), near + 1):
        given(distance)
        add_place(place_at(zn - distance))
    for i in (0, 1):

        @pl.when(k == 1)
        def _():
            for piece in range(PIECES):
                ring(near, i, piece, True).wait_recv()
                across(near + 1, i, piece, False).start()

        @pl.when(k == 0)
        def _():
            for piece in range(PIECES):
                across(near + 1, i, piece, True).wait_recv()

        add_stream(place_at(near + 1), i)

    @pl.when((section == 1) & (r == 0))
    def _():
        select_send().wait_recv()

    for first in range(0, 2 * zn, 4):
        bias_row[0:1, pl.ds(first * shard, 4 * shard)] = jnp.concatenate(
            [bias_of(slot) for slot in range(first, first + 4)], axis=1
        )

    def chunk_rows(chunk):
        return pl.ds(chunk * rows, rows)

    def forward(tick, chunk, landing):
        at = chunk_rows(chunk)
        return pltpu.make_async_remote_copy(
            src_ref=prod.at[tick, at],
            dst_ref=landing.at[tick, at],
            send_sem=hop_send.at[tick, chunk],
            recv_sem=hop_recv.at[tick, chunk],
            device_id=after,
            device_id_type=MESH,
        )

    def record(tick, chunk):
        at = chunk_rows(chunk)
        return pltpu.make_async_remote_copy(
            src_ref=prod.at[tick, at],
            dst_ref=result.at[tick, at],
            send_sem=record_send.at[tick, chunk],
            recv_sem=record_recv.at[tick, chunk],
            device_id=last_to,
            device_id_type=MESH,
        )

    def hand_back(tick, chunk):
        at = chunk_rows(chunk)
        return pltpu.make_async_remote_copy(
            src_ref=arr.at[tick, at],
            dst_ref=result.at[tick, at],
            send_sem=record_send.at[tick, chunk],
            recv_sem=record_recv.at[tick, chunk],
            device_id=swapped,
            device_id_type=MESH,
        )

    result = out.at[0]

    def send_on(tick, chunk):
        @pl.when(moves)
        def _():
            forward(tick, chunk, result).start()

        @pl.when(stays)
        def _():
            @pl.when(tick < TICKS - 1)
            def _():
                forward(tick, chunk, arr).start()

            @pl.when((tick == TICKS - 1) | (r == 0))
            def _():
                record(tick, chunk).start()

    for chunk in range(CHUNKS):
        prod[0, chunk_rows(chunk)] = acc[chunk_rows(chunk), :].astype(jnp.bfloat16)
        send_on(0, chunk)

    wide = 256

    def step(tick, chunk):
        at = chunk_rows(chunk)

        @pl.when(stays)
        def _():
            forward(tick - 1, chunk, result).wait_recv()
            cur[...] = out[0, tick - 1, at, :]

        @pl.when(moves)
        def _():
            forward(tick - 1, chunk, arr).wait_recv()
            cur[...] = arr[tick - 1, at, :]

            @pl.when(r == 0)
            def _():
                hand_back(tick - 1, chunk).start()

        @pl.when((section == 0) & (r == 0))
        def _():
            cur[...] = sel[tick - 1, at, :]

        @pl.when((section == 1) & (r == 0))
        def _():
            cur[...] = sel_far[tick - 1, at, :]

        normed, widened = normalize(cur[...], gain_row, shift_row)
        for low in range(0, width, wide):
            preact = rows_times(normed, win[low : low + wide, :]) + bias_row[0:1, low : low + wide]
            hid[:, low : low + wide] = activate(preact).astype(jnp.bfloat16)
        for low in range(0, depth, wide):
            mixed = jnp.dot(
                hid[...], wout[:, low : low + wide], preferred_element_type=jnp.float32
            )
            prod[tick, at, low : low + wide] = (
                widened[:, low : low + wide] + mixed + out_row[:, low : low + wide]
            ).astype(jnp.bfloat16)

        send_on(tick, chunk)

    @pl.loop(1, TICKS)
    def _(tick):
        for chunk in range(CHUNKS):
            step(tick, chunk)

    @pl.when(moves)
    def _():
        for tick in range(TICKS):
            for chunk in range(CHUNKS):
                record(tick, chunk).wait_recv()
                forward(tick, chunk, result).wait_send()
                if tick < TICKS - 1:

                    @pl.when(r == 0)
                    def _():
                        hand_back(tick, chunk).wait_send()

    @pl.when(stays)
    def _():
        for tick in range(TICKS):
            for chunk in range(CHUNKS):
                if tick == TICKS - 1:
                    forward(tick, chunk, result).wait_recv()
                    record(tick, chunk).wait_send()
                else:
                    forward(tick, chunk, arr).wait_send()

                    @pl.when(r == 0)
                    def _():
                        record(tick, chunk).wait_send()

    @pl.when(moves)
    def _():
        for i in range(OWN):
            own_remote(i, 2 * z + r).wait_send()

    @pl.when((section == 0) & (r == 1))
    def _():
        select_send().wait_send()

    for i, mine in ((0, stays), (1, moves)):
        for piece in range(PIECES):

            @pl.when(mine)
            def _():
                across(0, i, piece, False).wait_send()

            for hop in range(near):
                ring(hop, i, piece, False).wait_send()
                across(hop + 1, i, piece, False).wait_send()

            @pl.when(k == 1)
            def _():
                ring(near, i, piece, False).wait_send()
                across(near + 1, i, piece, False).wait_send()


def shards(
    section_inputs, w_in, in_bias, w_out, out_bias, norm_gain, norm_bias, patches, plan, *, yn, zn
):
    tokens, depth = section_inputs.shape[1:]
    shard = w_in.shape[1]
    width = 2 * zn * shard
    anywhere = pl.BlockSpec(memory_space=pl.ANY)
    half = zn // 2
    dma = pltpu.SemaphoreType.DMA
    return pl.pallas_call(
        functools.partial(block_kernel, yn, zn),
        out_shape=pltpu.VMEM((1, TICKS, tokens, depth), jnp.bfloat16),
        in_specs=[anywhere] * 8 + [pl.BlockSpec(memory_space=pltpu.SMEM)],
        out_specs=pl.BlockSpec(memory_space=pltpu.VMEM),
        scratch_shapes=[
            pltpu.VMEM((tokens, depth), jnp.bfloat16),
            pltpu.VMEM((width, depth), jnp.bfloat16),
            pltpu.VMEM((width, depth), jnp.bfloat16),
            pltpu.VMEM((1, depth), jnp.float32),
            pltpu.VMEM((1, depth), jnp.float32),
            pltpu.VMEM((1, depth), jnp.float32),
            pltpu.VMEM((2 * zn, 1, shard), jnp.bfloat16),
            pltpu.VMEM((8, width), jnp.float32),
            pltpu.VMEM(patches.shape, jnp.bfloat16),
            pltpu.VMEM((TICKS - 1, tokens, depth), jnp.bfloat16),
            pltpu.VMEM((TICKS - 1, tokens, depth), jnp.bfloat16),
            pltpu.VMEM((tokens // CHUNKS, depth), jnp.bfloat16),
            pltpu.VMEM((tokens, depth), jnp.bfloat16),
            pltpu.VMEM((tokens, depth), jnp.float32),
            pltpu.VMEM((tokens // CHUNKS, width), jnp.bfloat16),
            pltpu.VMEM((TICKS, tokens, depth), jnp.bfloat16),
            pltpu.VMEM((TICKS - 1, tokens, depth), jnp.bfloat16),
            dma((OWN,)),
            dma((OWN,)),
            dma((half, 2, PIECES)),
            dma((half, 2, PIECES)),
            dma((half + 1, 2, PIECES)),
            dma((half + 1, 2, PIECES)),
            dma((1,)),
            dma((1,)),
            dma((1,)),
            dma((TICKS, CHUNKS)),
            dma((TICKS, CHUNKS)),
            dma((TICKS, CHUNKS)),
            dma((TICKS, CHUNKS)),
        ],
        compiler_params=pltpu.CompilerParams(collective_id=0, has_side_effects=True),
    )(section_inputs, w_in, w_out, in_bias, out_bias, norm_gain, norm_bias, patches, plan)


def solution(mesh):
    placed = (
        P("section", "tensor", None),
        P("section", "tensor", None),
        P("section", "tensor"),
        P("section", "tensor", None),
        P("section", None),
        P("section", None),
        P("section", None),
        P(None, "tensor", None),
        P(),
    )
    return jax.shard_map(
        functools.partial(
            shards, yn=mesh.shape["section"] // 2, zn=mesh.shape["tensor"] // 2
        ),
        mesh=mesh,
        in_specs=placed,
        out_specs=P("section", None, "tensor", None),
        check_vma=False,
    )
```

```python
import functools

import jax
import jax.numpy as jnp
from jax import lax
from jax.experimental import pallas as pl
from jax.experimental.pallas import tpu as pltpu
from jax.sharding import PartitionSpec as P

TICKS = 4
CHUNKS = 2
MESH = pl.DeviceIdType.MESH

norm_floor = 0.1
gelu_slope = 1.702

OWN = 7
PIECES = 3


def normalize(current, gain_row, shift_row):
    widened = current.astype(jnp.float32)
    average = jnp.mean(widened, axis=-1, keepdims=True)
    centered = widened - average
    variance = jnp.mean(centered * centered, axis=-1, keepdims=True)
    normed = (centered * lax.rsqrt(variance + norm_floor) * gain_row + shift_row).astype(
        jnp.bfloat16
    )
    return (normed, widened)


def activate(preact):
    return preact * jax.nn.sigmoid(gelu_slope * preact)


def rows_times(normed, rows):
    return lax.dot_general(
        normed, rows, (((1,), (1,)), ((), ())), preferred_element_type=jnp.float32
    )


def block_kernel(
    yn, zn,
    x_in, w_in, w_out, bias_in, add_in, gain_in, shift_in, patches_in, plan, out,
    x0, win, wout, add, gain, shift, bias, bias_row, pat, sel, sel_far, cur, normed0, acc, hid, prod, arr,
    own_sem, own_send, ring_send, ring_recv, core_send, core_recv,
    pat_sem, sel_send, sel_recv, hop_send, hop_recv, record_send, record_recv,
):
    section = lax.axis_index("section")
    tensor = lax.axis_index("tensor")
    k = lax.rem(section, 2)
    y = lax.div(section, 2)
    r = lax.rem(tensor, 2)
    z = lax.div(tensor, 2)
    tokens, depth = x0.shape
    shard = w_in.shape[1]
    width = win.shape[0]
    near = (zn - 1) // 2
    rows = tokens // CHUNKS

    def device(y, k, z, r):
        return (2 * y + k, 2 * z + r)

    onward = device(y, k, lax.rem(z + 1 + k * (zn - 2), zn), r)
    inward = device(y, k, lax.rem(z + zn - 1 - k * (zn - 2), zn), r)
    sibling = device(y, 1 - k, z, r)
    swapped = device(y, r, z, k)
    after = device(lax.rem(y + r, yn), k, z, 1 - r)
    before = device(lax.rem(y + yn - 1 + r, yn), k, z, 1 - r)
    last_to = device(lax.rem(y + r, yn), 1 - r, z, k)
    last_from = device(lax.rem(y + yn - 1 + k, yn), r, z, 1 - k)
    stays = r == k
    moves = r != k

    def slot_ref(piece, slot):
        if piece == 0:
            return bias.at[slot]
        whole = win if piece == 1 else wout
        return whole.at[pl.ds(pl.multiple_of(slot * shard, shard), shard)]

    own = 2 * z + k
    sources = (
        bias_in,
        w_in.at[0],
        w_out.at[0],
        add_in,
        gain_in,
        shift_in,
        x_in.at[0],
    )

    def own_targets(slot):
        return tuple(slot_ref(piece, slot) for piece in range(PIECES)) + (
            add,
            gain,
            shift,
            x0,
        )

    def own_local(i):
        return pltpu.make_async_copy(sources[i], own_targets(own)[i], own_sem.at[i])

    def own_remote(i, slot):
        return pltpu.make_async_remote_copy(
            src_ref=sources[i],
            dst_ref=own_targets(slot)[i],
            send_sem=own_send.at[i],
            recv_sem=own_sem.at[i],
            device_id=swapped,
            device_id_type=MESH,
        )

    def own_wait(i):
        @pl.when(stays)
        def _():
            own_local(i).wait()

        @pl.when(moves)
        def _():
            own_remote(i, own).wait_recv()

    def patch_load():
        return pltpu.make_async_copy(patches_in, pat, pat_sem.at[0])

    @pl.when(stays)
    def _():
        for i in range(OWN):
            own_local(i).start()

    @pl.when(section == 0)
    def _():
        patch_load().start()

    barrier = pltpu.get_barrier_semaphore()

    def greet(partner):
        pl.semaphore_signal(barrier, inc=1, device_id=partner, device_id_type=MESH)

    for sender in (inward, sibling, before):
        greet(sender)

    @pl.when(moves)
    def _():
        greet(swapped)

    @pl.when((r == 1) & (k == 0))
    def _():
        greet(last_from)

    pl.semaphore_wait(barrier, 3 + r + k - r * k)

    @pl.when(moves)
    def _():
        for i in range(OWN):
            own_remote(i, 2 * z + r).start()

    first_stream = (r, 1 - r)

    def place_at(distance):
        return lax.rem(z + lax.rem(k * 2 * distance + zn - distance, zn), zn)

    def ring(hop, i, piece, arriving):
        ref = slot_ref(piece, 2 * place_at(hop + 1 if arriving else hop) + first_stream[i])
        return pltpu.make_async_remote_copy(
            src_ref=ref,
            dst_ref=ref,
            send_sem=ring_send.at[hop, i, piece],
            recv_sem=ring_recv.at[hop, i, piece],
            device_id=onward,
            device_id_type=MESH,
        )

    def across(distance, i, piece, arriving):
        place = place_at((zn - distance) % zn if arriving else distance)
        ref = slot_ref(piece, 2 * place + first_stream[i])
        return pltpu.make_async_remote_copy(
            src_ref=ref,
            dst_ref=ref,
            send_sem=core_send.at[distance, i, piece],
            recv_sem=core_recv.at[distance, i, piece],
            device_id=sibling,
            device_id_type=MESH,
        )

    for i, mine in ((0, stays), (1, moves)):
        for piece in range(PIECES):

            @pl.when(mine)
            def _():
                own_wait(piece)
                across(0, i, piece, False).start()

            @pl.when(jnp.logical_not(mine))
            def _():
                across(0, i, piece, True).wait_recv()

            ring(0, i, piece, False).start()

    for i in range(PIECES, OWN):
        own_wait(i)
    gain_row = gain[...]
    shift_row = shift[...]
    out_row = add[...]
    normed, widened = normalize(x0[...], gain_row, shift_row)
    normed0[...] = normed
    acc[...] = widened + out_row

    def bias_of(slot):
        return bias[slot].astype(jnp.float32)

    def add_rows(at, bias_here):
        preact = rows_times(normed0[...], win[at, :]) + bias_here
        hidden = activate(preact).astype(jnp.bfloat16)
        acc[...] += jnp.dot(hidden, wout[at, :], preferred_element_type=jnp.float32)

    def add_place(place):
        both = jnp.concatenate(
            [bias_of(2 * place), bias_of(2 * place + 1)], axis=1
        )
        add_rows(pl.ds(pl.multiple_of(place * 2 * shard, 2 * shard), 2 * shard), both)

    def add_stream(place, i):
        slot = 2 * place + first_stream[i]
        add_rows(pl.ds(pl.multiple_of(slot * shard, shard), shard), bias_of(slot))

    def take(hop):
        for i in (0, 1):
            for piece in range(PIECES):
                ring(hop, i, piece, True).wait_recv()
                if hop + 1 < near:
                    ring(hop + 1, i, piece, False).start()
                else:

                    @pl.when(k == 1)
                    def _():
                        ring(hop + 1, i, piece, False).start()

                across(hop + 1, i, piece, False).start()

    def given(distance):
        for i in (0, 1):
            for piece in range(PIECES):
                across(distance, i, piece, True).wait_recv()

    def select_send():
        return pltpu.make_async_remote_copy(
            src_ref=sel,
            dst_ref=sel_far,
            send_sem=sel_send.at[0],
            recv_sem=sel_recv.at[0],
            device_id=swapped,
            device_id_type=MESH,
        )

    add_place(z)
    for hop in range(near):
        take(hop)
        add_place(place_at(hop + 1))
        if hop == 1:

            @pl.when(section == 0)
            def _():
                patch_load().wait()
                for i in range(TICKS - 1):
                    sel[i] = pat[plan[i]]

            @pl.when((section == 0) & (r == 1))
            def _():
                select_send().start()

        if hop >= 2:
            given(hop - 1)
            add_place(place_at(zn - hop + 1))
    for distance in range(max(1, near - 1), near + 1):
        given(distance)
        add_place(place_at(zn - distance))
    for i in (0, 1):

        @pl.when(k == 1)
        def _():
            for piece in range(PIECES):
                ring(near, i, piece, True).wait_recv()
                across(near + 1, i, piece, False).start()

        @pl.when(k == 0)
        def _():
            for piece in range(PIECES):
                across(near + 1, i, piece, True).wait_recv()

        add_stream(place_at(near + 1), i)

    @pl.when((section == 1) & (r == 0))
    def _():
        select_send().wait_recv()

    for first in range(0, 2 * zn, 4):
        bias_row[0:1, pl.ds(first * shard, 4 * shard)] = jnp.concatenate(
            [bias_of(slot) for slot in range(first, first + 4)], axis=1
        )

    def chunk_rows(chunk):
        return pl.ds(chunk * rows, rows)

    def forward(tick, chunk, landing):
        at = chunk_rows(chunk)
        return pltpu.make_async_remote_copy(
            src_ref=prod.at[tick, at],
            dst_ref=landing.at[tick, at],
            send_sem=hop_send.at[tick, chunk],
            recv_sem=hop_recv.at[tick, chunk],
            device_id=after,
            device_id_type=MESH,
        )

    def record(tick, chunk):
        at = chunk_rows(chunk)
        return pltpu.make_async_remote_copy(
            src_ref=prod.at[tick, at],
            dst_ref=result.at[tick, at],
            send_sem=record_send.at[tick, chunk],
            recv_sem=record_recv.at[tick, chunk],
            device_id=last_to,
            device_id_type=MESH,
        )

    def hand_back(tick, chunk):
        at = chunk_rows(chunk)
        return pltpu.make_async_remote_copy(
            src_ref=arr.at[tick, at],
            dst_ref=result.at[tick, at],
            send_sem=record_send.at[tick, chunk],
            recv_sem=record_recv.at[tick, chunk],
            device_id=swapped,
            device_id_type=MESH,
        )

    result = out.at[0]

    def send_on(tick, chunk):
        @pl.when(moves)
        def _():
            forward(tick, chunk, result).start()

        @pl.when(stays)
        def _():
            @pl.when(tick < TICKS - 1)
            def _():
                forward(tick, chunk, arr).start()

            @pl.when((tick == TICKS - 1) | (tick == 1) | (r == 0))
            def _():
                record(tick, chunk).start()

    for chunk in range(CHUNKS):
        prod[0, chunk_rows(chunk)] = acc[chunk_rows(chunk), :].astype(jnp.bfloat16)
        send_on(0, chunk)

    wide = 256

    def step(tick, chunk):
        at = chunk_rows(chunk)

        @pl.when(stays)
        def _():
            forward(tick - 1, chunk, result).wait_recv()
            cur[...] = out[0, tick - 1, at, :]

        @pl.when(moves)
        def _():
            forward(tick - 1, chunk, arr).wait_recv()
            cur[...] = arr[tick - 1, at, :]

            @pl.when((r == 0) & (tick != 2))
            def _():
                hand_back(tick - 1, chunk).start()

        @pl.when((section == 0) & (r == 0))
        def _():
            cur[...] = sel[tick - 1, at, :]

        @pl.when((section == 1) & (r == 0))
        def _():
            cur[...] = sel_far[tick - 1, at, :]

        normed, widened = normalize(cur[...], gain_row, shift_row)
        for low in range(0, width, wide):
            preact = rows_times(normed, win[low : low + wide, :]) + bias_row[0:1, low : low + wide]
            hid[:, low : low + wide] = activate(preact).astype(jnp.bfloat16)
        for low in range(0, depth, wide):
            mixed = jnp.dot(
                hid[...], wout[:, low : low + wide], preferred_element_type=jnp.float32
            )
            prod[tick, at, low : low + wide] = (
                widened[:, low : low + wide] + mixed + out_row[:, low : low + wide]
            ).astype(jnp.bfloat16)

        send_on(tick, chunk)

    @pl.loop(1, TICKS)
    def _(tick):
        for chunk in range(CHUNKS):
            step(tick, chunk)

    @pl.when(moves)
    def _():
        for tick in range(TICKS):
            for chunk in range(CHUNKS):
                record(tick, chunk).wait_recv()
                forward(tick, chunk, result).wait_send()
                if tick < TICKS - 1 and tick != 1:

                    @pl.when(r == 0)
                    def _():
                        hand_back(tick, chunk).wait_send()

    @pl.when(stays)
    def _():
        for tick in range(TICKS):
            for chunk in range(CHUNKS):
                if tick == TICKS - 1:
                    forward(tick, chunk, result).wait_recv()
                    record(tick, chunk).wait_send()
                else:
                    forward(tick, chunk, arr).wait_send()

                    @pl.when((r == 0) | (tick == 1))
                    def _():
                        record(tick, chunk).wait_send()

    @pl.when(moves)
    def _():
        for i in range(OWN):
            own_remote(i, 2 * z + r).wait_send()

    @pl.when((section == 0) & (r == 1))
    def _():
        select_send().wait_send()

    for i, mine in ((0, stays), (1, moves)):
        for piece in range(PIECES):

            @pl.when(mine)
            def _():
                across(0, i, piece, False).wait_send()

            for hop in range(near):
                ring(hop, i, piece, False).wait_send()
                across(hop + 1, i, piece, False).wait_send()

            @pl.when(k == 1)
            def _():
                ring(near, i, piece, False).wait_send()
                across(near + 1, i, piece, False).wait_send()


def shards(
    section_inputs, w_in, in_bias, w_out, out_bias, norm_gain, norm_bias, patches, plan, *, yn, zn
):
    tokens, depth = section_inputs.shape[1:]
    shard = w_in.shape[1]
    width = 2 * zn * shard
    anywhere = pl.BlockSpec(memory_space=pl.ANY)
    half = zn // 2
    dma = pltpu.SemaphoreType.DMA
    return pl.pallas_call(
        functools.partial(block_kernel, yn, zn),
        out_shape=pltpu.VMEM((1, TICKS, tokens, depth), jnp.bfloat16),
        in_specs=[anywhere] * 8 + [pl.BlockSpec(memory_space=pltpu.SMEM)],
        out_specs=pl.BlockSpec(memory_space=pltpu.VMEM),
        scratch_shapes=[
            pltpu.VMEM((tokens, depth), jnp.bfloat16),
            pltpu.VMEM((width, depth), jnp.bfloat16),
            pltpu.VMEM((width, depth), jnp.bfloat16),
            pltpu.VMEM((1, depth), jnp.float32),
            pltpu.VMEM((1, depth), jnp.float32),
            pltpu.VMEM((1, depth), jnp.float32),
            pltpu.VMEM((2 * zn, 1, shard), jnp.bfloat16),
            pltpu.VMEM((8, width), jnp.float32),
            pltpu.VMEM(patches.shape, jnp.bfloat16),
            pltpu.VMEM((TICKS - 1, tokens, depth), jnp.bfloat16),
            pltpu.VMEM((TICKS - 1, tokens, depth), jnp.bfloat16),
            pltpu.VMEM((tokens // CHUNKS, depth), jnp.bfloat16),
            pltpu.VMEM((tokens, depth), jnp.bfloat16),
            pltpu.VMEM((tokens, depth), jnp.float32),
            pltpu.VMEM((tokens // CHUNKS, width), jnp.bfloat16),
            pltpu.VMEM((TICKS, tokens, depth), jnp.bfloat16),
            pltpu.VMEM((TICKS - 1, tokens, depth), jnp.bfloat16),
            dma((OWN,)),
            dma((OWN,)),
            dma((half, 2, PIECES)),
            dma((half, 2, PIECES)),
            dma((half + 1, 2, PIECES)),
            dma((half + 1, 2, PIECES)),
            dma((1,)),
            dma((1,)),
            dma((1,)),
            dma((TICKS, CHUNKS)),
            dma((TICKS, CHUNKS)),
            dma((TICKS, CHUNKS)),
            dma((TICKS, CHUNKS)),
        ],
        compiler_params=pltpu.CompilerParams(collective_id=0, has_side_effects=True),
    )(section_inputs, w_in, w_out, in_bias, out_bias, norm_gain, norm_bias, patches, plan)


def solution(mesh):
    placed = (
        P("section", "tensor", None),
        P("section", "tensor", None),
        P("section", "tensor"),
        P("section", "tensor", None),
        P("section", None),
        P("section", None),
        P("section", None),
        P(None, "tensor", None),
        P(),
    )
    return jax.shard_map(
        functools.partial(
            shards, yn=mesh.shape["section"] // 2, zn=mesh.shape["tensor"] // 2
        ),
        mesh=mesh,
        in_specs=placed,
        out_specs=P("section", None, "tensor", None),
        check_vma=False,
    )
```
